32 devices in a mesh: rep: 4 (over x, core), shard: 8 (over z, y).
Axes of the slice: x: 2, y: 2, z: 4, core: 2. Of those that a mesh axis runs over, the one named last changes fastest.
Arguments:
- inputs: bfloat16 [32, 1024, 1024], P(('rep', 'shard')), may hold values from -6 to 6
- cotangent: bfloat16 [32, 1024, 1024], P(('rep', 'shard')), may hold values from -6 to 6
- lengths: int32 [32], P(('rep', 'shard')), may hold values from 256 to 1024, as said below
- adapter_ids: int32 [32], P(('rep', 'shard')), may hold values from 0 to 7
- gain_one: float32 [1024], replicated, may hold values from 0.25 to 1.75
- gain_two: float32 [1024], replicated, may hold values from 0.25 to 1.75
- qkv_weight: bfloat16 [1024, 3072], P('shard'), may hold values from -0.1875 to 0.1875
- out_weight: bfloat16 [1024, 1024], P('shard'), may hold values from -0.75 to 0.75
- up_weight: bfloat16 [1024, 4096], P('shard'), may hold values from -0.1875 to 0.1875
- down_weight: bfloat16 [4096, 1024], P('shard'), may hold values from -0.09375 to 0.09375
- adapter_down: bfloat16 [1024, 512], P('shard'), may hold values from -0.1875 to 0.1875
- adapter_up: bfloat16 [1024, 512], P('shard'), may hold values from -1.5 to 1.5
Outputs:
- layer_output: bfloat16 [32, 1024, 1024], P(('rep', 'shard'))
- input_grad: bfloat16 [32, 1024, 1024], P(('rep', 'shard'))
- adapter_down_grad: float32 [1024, 512], P('shard')
- adapter_up_grad: float32 [1024, 512], P('shard')
The draws below stay inside these ranges and needn't reach their ends.
Inputs may be any that keep to these rules, and one draw needn't show every extreme that they name: `lengths`: every draw has a slot of length 1024.
All inputs are finite; a program needn't handle non-finite values.
Results may differ from the reference program's by a relative error of at most 0.015.
The reference program's roundings to bfloat16 on the way count: a program that leaves them out, or rounds other values in their place, can miss the bound.
Values may be sent and summed in bfloat16 or wider, within the bound.
A program may use at most 256 MiB of HBM per device.

```python
import jax
import jax.numpy as jnp
from jax import lax

D = 1024
HEADS = 16
HEAD = 64
FF = 4096
RANK = 16
ADAPTERS = 8
SEQ = 1024
MIN_LEN = 256
SLOTS = 32
NCOL = 512


def draw_lengths(key, part):
    drawn = jax.random.randint(jax.random.fold_in(key, 11), (SLOTS,), MIN_LEN, SEQ + 1)
    chosen = jax.random.randint(jax.random.fold_in(key, 12), (), 0, SLOTS)
    return jnp.where(lax.iota(jnp.int32, SLOTS) == chosen, SEQ, drawn).astype(jnp.int32)


def with_ends(values, own_key, low, high):
    shape = values.shape
    index_at = [jax.random.randint(jax.random.fold_in(own_key, axis), (), 0, shape[axis]) for axis in range(len(shape))]
    values = values.at[tuple(index_at)].set(low)
    longest = shape.index(max(shape))
    index_at[longest] = (index_at[longest] + 1) % shape[longest]
    return values.at[tuple(index_at)].set(high)


def levels(own_key, extent, shards, low, high):
    factor_of, own = 1.0, jax.random.fold_in(own_key, 6)
    for axis_at, parts in shards:
        steps = jnp.exp(jax.random.uniform(jax.random.fold_in(own, axis_at), (parts,), jnp.float32, low / len(shards), high / len(shards)))
        factor_of = factor_of * jnp.repeat(steps, extent[axis_at] // parts).reshape([-1 if axis == axis_at else 1 for axis in range(len(extent))])
    return factor_of


def gaussian(key, extent, scale, most, shards=(), dtype=jnp.bfloat16):
    entries = jax.random.normal(key, extent, jnp.float32) * scale
    if len(shards) > 0:
        entries = levels(key, extent, shards, -0.22, 0.18) * entries
    return jnp.clip(entries, min=-most, max=most).astype(dtype)


def setup_inputs(seed: int = 0) -> dict:
    splits = jax.random.split(jax.random.key(seed), 13)
    inputs = gaussian(splits[0], (SLOTS, SEQ, D), 1.0, 6.0, ((0, 32),))
    cotangent = gaussian(splits[1], (SLOTS, SEQ, D), 1.0, 6.0, ((0, 32),))
    lengths = draw_lengths(jax.random.fold_in(splits[12], 71), 0)
    adapter_ids = with_ends(jax.random.randint(splits[3], (SLOTS,), 0, ADAPTERS), jax.random.fold_in(splits[3], 1), 0, ADAPTERS - 1).astype(jnp.int32)
    gain_one = jnp.clip(1.0 + 0.15 * jax.random.normal(splits[4], (D,), jnp.float32), 0.25, 1.75)
    gain_two = jnp.clip(1.0 + 0.15 * jax.random.normal(splits[5], (D,), jnp.float32), 0.25, 1.75)
    qkv_weight = gaussian(splits[6], (D, 3 * D), D ** -0.5, 0.1875, ((0, 8),))
    out_weight = gaussian(splits[7], (D, D), (D // 16) ** -0.5, 0.75, ((0, 8),))
    up_weight = gaussian(splits[8], (D, FF), D ** -0.5, 0.1875, ((0, 8),))
    down_weight = gaussian(splits[9], (FF, D), FF ** -0.5, 0.09375, ((0, 8),))
    adapter_down = gaussian(splits[10], (D, NCOL), D ** -0.5, 0.1875, ((0, 8),))
    adapter_up = gaussian(splits[11], (D, NCOL), RANK ** -0.5, 1.5, ((0, 8),))
    return dict(inputs=inputs, cotangent=cotangent, lengths=lengths, adapter_ids=adapter_ids, gain_one=gain_one, gain_two=gain_two, qkv_weight=qkv_weight, out_weight=out_weight, up_weight=up_weight, down_weight=down_weight, adapter_down=adapter_down, adapter_up=adapter_up)


@jax.custom_vjp
def low(v):
    return lax.optimization_barrier(v.astype(jnp.bfloat16)).astype(jnp.float32)

@jax.custom_vjp
def low_back(v):
    return v

def low_keep(v):
    return (low(v), None)

def low_pass(kept, grad):
    return (grad,)

def back_keep(v):
    return (v, None)

def back_low(kept, grad):
    return (low(grad),)
low.defvjp(low_keep, low_pass)
low_back.defvjp(back_keep, back_low)
EPS = 1e-05
HIGH = lax.Precision.HIGHEST

def layer_norm(vector, gain):
    center = vector - lax.optimization_barrier(jnp.mean(vector, axis=-1, keepdims=True))
    spread = lax.optimization_barrier(jnp.mean(center * center, axis=-1, keepdims=True))
    return center * lax.rsqrt(spread + EPS) * gain

def product(left, right):
    return jnp.dot(left, right, precision=HIGH)

def forward(tokens, adapter_down, adapter_up, length, adapter, frozen):
    gain_one, gain_two, qkv_weight, out_weight, up_weight, down_weight = frozen
    seq = tokens.shape[0]
    width = HEADS * HEAD
    first = (adapter * (4 * RANK)).astype(jnp.int32)
    local_down = lax.dynamic_slice_in_dim(adapter_down, first, 4 * RANK, 1)
    local_up = lax.dynamic_slice_in_dim(adapter_up, first, 4 * RANK, 1)
    normed = low(layer_norm(tokens, gain_one))
    inner = low(low_back(product(normed, local_down[:, :3 * RANK])))
    extra = jnp.concatenate([product(inner[:, j * RANK:(j + 1) * RANK], local_up[:, j * RANK:(j + 1) * RANK].T) for j in range(3)], axis=1)
    projected = low(low_back(product(normed, qkv_weight) + extra))
    queries = projected[:, :width].reshape(seq, HEADS, HEAD)
    keys_all = projected[:, width:2 * width].reshape(seq, HEADS, HEAD)
    values_all = projected[:, 2 * width:].reshape(seq, HEADS, HEAD)
    scores = low_back(jnp.einsum('qhd,khd->hqk', queries, keys_all, precision=HIGH) * HEAD ** (-0.5))
    positions = lax.iota(jnp.int32, seq)
    causal = positions[:, None] >= positions[None, :]
    scores = jnp.where(causal[None], scores, -1e+30)
    probs = low(jax.nn.softmax(scores, axis=-1))
    context = jnp.einsum('hqk,khd->qhd', probs, values_all, precision=HIGH).reshape(seq, width)
    context = low(low_back(context))
    inner_out = low(low_back(product(context, local_down[:, 3 * RANK:])))
    attended = low_back(product(context, out_weight) + product(inner_out, local_up[:, 3 * RANK:].T))
    hidden = tokens + attended
    normed_two = low(layer_norm(hidden, gain_two))
    pre = low_back(product(normed_two, up_weight))
    active = low(jax.nn.gelu(pre, approximate=True))
    mlp = low_back(product(active, down_weight))
    valid = (positions < length).astype(jnp.float32)[:, None]
    return (hidden + mlp) * valid

def reference(inputs, cotangent, lengths, adapter_ids, gain_one, gain_two, qkv_weight, out_weight, up_weight, down_weight, adapter_down, adapter_up):
    frozen = (gain_one.astype(jnp.float32), gain_two.astype(jnp.float32), qkv_weight.astype(jnp.float32), out_weight.astype(jnp.float32), up_weight.astype(jnp.float32), down_weight.astype(jnp.float32))
    down_float = adapter_down.astype(jnp.float32)
    up_float = adapter_up.astype(jnp.float32)

    def one_slot(carry, slot):
        tokens, slot_cot, length, adapter = slot

        def run_layer(token_vals, down_cols, up_cols):
            return forward(token_vals, down_cols, up_cols, length, adapter, frozen)
        output, pull = jax.vjp(run_layer, tokens.astype(jnp.float32), down_float, up_float)
        grad_input, grad_down, grad_up = pull(slot_cot.astype(jnp.float32))
        return ((carry[0] + grad_down, carry[1] + grad_up), (output.astype(jnp.bfloat16), grad_input.astype(jnp.bfloat16)))
    start = (jnp.zeros_like(down_float), jnp.zeros_like(up_float))
    totals, results = lax.scan(one_slot, start, (inputs, cotangent, lengths, adapter_ids))
    return (results[0], results[1], totals[0], totals[1])
```

```python
import functools

import jax
import jax.numpy as jnp
from jax import lax
from jax.experimental import pallas as pl
from jax.experimental.pallas import tpu as pltpu
from jax.sharding import PartitionSpec as P


HEADS = 16
RANK = 16
ADAPTERS = 8


EPS = 1e-05
HIGH = lax.Precision.HIGHEST


def layer_norm(vector, gain):
    center = vector - jnp.mean(vector, axis=-1, keepdims=True)
    spread = jnp.mean(center * center, axis=-1, keepdims=True)
    return center * lax.rsqrt(spread + EPS) * gain


def norm_back(vector, gain, grad_normed):

    def apply_norm(values_in):
        return layer_norm(values_in, gain)

    pull = jax.vjp(apply_norm, vector)[1]
    return pull(grad_normed)[0]


def gelu_tanh(values_in):
    return jax.nn.gelu(values_in, approximate=True)


def gelu_back(pre, grad_active):
    pull = jax.vjp(gelu_tanh, pre)[1]
    return pull(grad_active)[0]


def dense(left, right):
    return jnp.dot(left, right, preferred_element_type=jnp.float32)


def dense_trans(left, right):
    return lax.dot_general(
        left, right, (((1,), (1,)), ((), ())), preferred_element_type=jnp.float32
    )


def dense_left(left, right):
    return lax.dot_general(
        left, right, (((0,), (0,)), ((), ())), preferred_element_type=jnp.float32
    )


def split_heads(projected):
    seq = projected.shape[0]
    width = projected.shape[1] // 3
    head_size = width // HEADS
    queries = projected[:, :width].reshape(seq, HEADS, head_size)
    keys_all = projected[:, width : 2 * width].reshape(seq, HEADS, head_size)
    values_all = projected[:, 2 * width :].reshape(seq, HEADS, head_size)
    return (queries, keys_all, values_all, head_size ** (-0.5))


def block_scores(queries, keys_all, start, block, scale):
    stop = start + block
    scores = (
        jnp.einsum(
            "qhd,khd->hqk", queries[start:stop], keys_all[:stop], preferred_element_type=jnp.float32
        )
        * scale
    )
    rows = start + lax.iota(jnp.int32, block)
    causal = rows[:, None] >= lax.iota(jnp.int32, stop)[None, :]
    return (scores, causal[None])


def attention_forward(projected):
    queries, keys_all, values_all, scale = split_heads(projected)
    seq = projected.shape[0]
    block = min(512, seq)
    pieces = []
    totals = []
    for start in range(0, seq, block):
        scores, causal = block_scores(queries, keys_all, start, block, scale)
        scores = jnp.where(causal, scores, -1e30)
        peak = jnp.max(scores, axis=-1, keepdims=True)
        expo = jnp.exp(scores - peak)
        total = jnp.sum(expo, axis=-1, keepdims=True)
        probs_low = (expo / total).astype(jnp.bfloat16)
        pieces.append(
            jnp.einsum(
                "hqk,khd->qhd",
                probs_low,
                values_all[: start + block],
                preferred_element_type=jnp.float32,
            )
        )
        totals.append(peak + jnp.log(total))
    context = jnp.concatenate(pieces, axis=0).reshape(seq, -1)
    return (context, jnp.concatenate(totals, axis=1))


def attention_backward(projected, log_total, grad_context):
    queries, keys_all, values_all, scale = split_heads(projected)
    seq = projected.shape[0]
    block = min(512, seq)
    grad_ctx = grad_context.reshape(queries.shape)
    grad_keys = jnp.zeros(queries.shape, jnp.float32)
    grad_values = jnp.zeros(queries.shape, jnp.float32)
    grad_queries = []
    for start in range(0, seq, block):
        stop = start + block
        scores, causal = block_scores(queries, keys_all, start, block, scale)
        probs = jnp.where(causal, jnp.exp(scores - log_total[:, start:stop]), 0.0)
        probs_low = probs.astype(jnp.bfloat16)
        ctx_block = grad_ctx[start:stop]
        grad_values = grad_values.at[:stop].add(
            jnp.einsum("hqk,qhd->khd", probs_low, ctx_block, preferred_element_type=jnp.float32)
        )
        grad_probs = jnp.einsum(
            "qhd,khd->hqk", ctx_block, values_all[:stop], preferred_element_type=jnp.float32
        )
        grad_scores = (
            probs * (grad_probs - jnp.sum(probs * grad_probs, axis=-1, keepdims=True))
        ).astype(jnp.bfloat16)
        grad_queries.append(
            jnp.einsum(
                "hqk,khd->qhd", grad_scores, keys_all[:stop], preferred_element_type=jnp.float32
            )
            * scale
        )
        grad_keys = grad_keys.at[:stop].add(
            jnp.einsum(
                "hqk,qhd->khd", grad_scores, queries[start:stop], preferred_element_type=jnp.float32
            )
            * scale
        )
    grad_q = jnp.concatenate(grad_queries, axis=0).reshape(seq, -1)
    return jnp.concatenate(
        [grad_q, grad_keys.reshape(seq, -1), grad_values.reshape(seq, -1)], axis=1
    )


def adapter_columns(weights, adapter):
    first = adapter * (4 * RANK)
    local_down = lax.dynamic_slice_in_dim(weights[4], first, 4 * RANK, 1)
    local_up = lax.dynamic_slice_in_dim(weights[5], first, 4 * RANK, 1)
    return (local_down, local_up)


def forward_slot(tokens, length, adapter, weights, gain_one, gain_two):
    qkv_weight, out_weight, up_weight, down_weight = (
        weights[0],
        weights[1],
        weights[2],
        weights[3],
    )
    local_down, local_up = adapter_columns(weights, adapter)
    seq = tokens.shape[0]
    token_vals = tokens.astype(jnp.float32)
    normed = layer_norm(token_vals, gain_one).astype(jnp.bfloat16)
    inner = dense(normed, local_down[:, : 3 * RANK]).astype(jnp.bfloat16)
    extra = jnp.concatenate(
        [
            dense_trans(inner[:, j * RANK : (j + 1) * RANK], local_up[:, j * RANK : (j + 1) * RANK])
            for j in range(3)
        ],
        axis=1,
    )
    projected = (dense(normed, qkv_weight) + extra).astype(jnp.bfloat16)
    context, log_total = attention_forward(projected)
    context_low = context.astype(jnp.bfloat16)
    inner_out = dense(context_low, local_down[:, 3 * RANK :]).astype(jnp.bfloat16)
    hidden = token_vals + (
        dense(context_low, out_weight) + dense_trans(inner_out, local_up[:, 3 * RANK :])
    )
    normed_two = layer_norm(hidden, gain_two).astype(jnp.bfloat16)
    pre = dense(normed_two, up_weight)
    active = gelu_tanh(pre).astype(jnp.bfloat16)
    mlp = dense(active, down_weight)
    valid = (lax.iota(jnp.int32, seq) < length).astype(jnp.float32)[:, None]
    output = ((hidden + mlp) * valid).astype(jnp.bfloat16)
    return (output, (normed, inner, projected, log_total, context_low, inner_out, hidden, pre))


def backward_slot(tokens, slot_cot, length, adapter, saved, weights, gain_one, gain_two):
    qkv_weight, out_weight, up_weight, down_weight = (
        weights[0],
        weights[1],
        weights[2],
        weights[3],
    )
    local_down, local_up = adapter_columns(weights, adapter)
    normed, inner, projected, log_total, context_low, inner_out, hidden, pre = saved
    seq = tokens.shape[0]
    width = projected.shape[1] // 3
    valid = (lax.iota(jnp.int32, seq) < length).astype(jnp.float32)[:, None]
    grad_out = slot_cot.astype(jnp.float32) * valid
    grad_mlp = grad_out.astype(jnp.bfloat16)
    grad_pre = gelu_back(pre, dense_trans(grad_mlp, down_weight)).astype(jnp.bfloat16)
    grad_hidden = grad_out + norm_back(hidden, gain_two, dense_trans(grad_pre, up_weight))
    grad_attended = grad_hidden.astype(jnp.bfloat16)
    grad_inner_out = dense(grad_attended, local_up[:, 3 * RANK :]).astype(jnp.bfloat16)
    up_out_grad = dense_left(grad_attended, inner_out)
    grad_context = (
        dense_trans(grad_attended, out_weight)
        + dense_trans(grad_inner_out, local_down[:, 3 * RANK :])
    ).astype(jnp.bfloat16)
    down_out_grad = dense_left(context_low, grad_inner_out)
    grad_projected = attention_backward(projected, log_total, grad_context).astype(jnp.bfloat16)
    grad_inner = jnp.concatenate(
        [
            dense(
                grad_projected[:, j * width : (j + 1) * width],
                local_up[:, j * RANK : (j + 1) * RANK],
            )
            for j in range(3)
        ],
        axis=1,
    ).astype(jnp.bfloat16)
    up_qkv_grad = jnp.concatenate(
        [
            dense_left(
                grad_projected[:, j * width : (j + 1) * width], inner[:, j * RANK : (j + 1) * RANK]
            )
            for j in range(3)
        ],
        axis=1,
    )
    grad_normed = dense_trans(grad_projected, qkv_weight) + dense_trans(
        grad_inner, local_down[:, : 3 * RANK]
    )
    down_qkv_grad = dense_left(normed, grad_inner)
    grad_input = grad_hidden + norm_back(tokens.astype(jnp.float32), gain_one, grad_normed)
    block_down = jnp.concatenate([down_qkv_grad, down_out_grad], axis=1)
    block_up = jnp.concatenate([up_qkv_grad, up_out_grad], axis=1)
    return (grad_input.astype(jnp.bfloat16), block_down, block_up)


def place_blocks(blocks, slot_ids):
    picks = (slot_ids[:, None] == lax.iota(jnp.int32, ADAPTERS)[None, :]).astype(jnp.float32)
    placed = jnp.einsum("sa,src->rac", picks, blocks, precision=HIGH)
    return placed.reshape(blocks.shape[1], ADAPTERS * blocks.shape[2])


MESH = pl.DeviceIdType.MESH

def mesh_split(n_rep, n_shard):
    zs = 4 if n_shard % 4 == 0 else n_shard
    return zs, n_shard // zs

def share_rows(rows):
    return max(16, rows * 3 // 8 // 16 * 16)

def chunk_list(shapes, width):
    out = []
    for w, (rows, cols) in enumerate(shapes):
        for r0 in range(0, rows, 128):
            for c0 in range(0, cols, width):
                out.append((w, r0, min(rows, 128), c0, min(width, cols)))
    return out

def gather_kernel(n_w, zs, ys, chunks, *refs):
    ins = refs[:n_w]
    outs = refs[n_w:2 * n_w]
    zsend, zrecv, ysend, yrecv, xsend, xrecv, csend, crecv, lsem = refs[2 * n_w:]
    r = lax.axis_index("rep")
    s = lax.axis_index("shard")
    z, y = s // ys, lax.rem(s, ys)
    core = lax.rem(r, 2)
    xp = lax.rem(r // 2, 2)
    sib = r + 1 - 2 * core
    par = r + 2 - 4 * xp
    zpeers = [lax.rem(z + k, zs) for k in range(1, zs)]
    ypeers = [lax.rem(y + k, ys) for k in range(1, ys)]
    peers = [(r, zz * ys + y) for zz in zpeers] + [(r, z * ys + yy) for yy in ypeers] + [(par, s), (sib, s)]
    local = []
    for w in range(n_w):
        cp = pltpu.make_async_copy(ins[w], outs[w].at[z, y], lsem.at[w])
        cp.start()
        local.append(cp)
    bar = pltpu.get_barrier_semaphore()
    for p in peers:
        pl.semaphore_signal(bar, inc=1, device_id=p, device_id_type=MESH)
    pl.semaphore_wait(bar, len(peers))

    def rdma(src, dst, ss, rs, dev):
        cp = pltpu.make_async_remote_copy(src_ref=src, dst_ref=dst, send_sem=ss, recv_sem=rs, device_id=dev, device_id_type=MESH)
        cp.start()

    def geom(t):
        w, r0, rows, c0, cols = chunks[t]
        a = share_rows(rows)
        half = cols // 2
        mine = pl.ds(pl.multiple_of(r0 + xp * a, 16), rows - a)
        excl = pl.ds(pl.multiple_of(r0 + xp * (rows - a), 16), a)
        missing = pl.ds(pl.multiple_of(r0 + (1 - xp) * (rows - a), 16), a)
        col = pl.ds(pl.multiple_of(c0 + core * half, 128), half)
        return w, a, half, rows, mine, excl, missing, col

    def wait_total(elems, sem):
        for out in outs:
            _, _, big_r, big_n = out.shape
            for lead in range(1, zs + 1):
                for take in range(big_r, 0, -16):
                    if elems % (lead * take * 128) == 0 and elems // (lead * take) <= big_n:
                        reg = out.at[pl.ds(0, lead), 0, pl.ds(0, take), pl.ds(0, elems // (lead * take))]
                        pltpu.make_async_copy(reg, reg, sem).wait()
                        return
        raise ValueError("no region")

    def stage_z(t):
        w, a, half, rows, mine, excl, missing, col = geom(t)
        for zz in zpeers:
            rdma(ins[w].at[mine, col], outs[w].at[z, y, mine, col], zsend.at[t], zrecv.at[t], (r, zz * ys + y))

    def stage_y(t):
        w, a, half, rows, mine, excl, missing, col = geom(t)
        wait_total((zs - 1) * (rows - a) * half, zrecv.at[t])
        for yy in ypeers:
            rdma(outs[w].at[:, y, mine, col], outs[w].at[:, y, mine, col], ysend.at[t], yrecv.at[t], (r, z * ys + yy))
        for zz in zpeers:
            rdma(outs[w].at[zz, y, excl, col], outs[w].at[zz, y, excl, col], xsend.at[t], xrecv.at[t], (par, s))
            rdma(outs[w].at[zz, y, mine, col], outs[w].at[zz, y, mine, col], csend.at[t], crecv.at[t], (sib, s))

    def stage_x(t):
        w, a, half, rows, mine, excl, missing, col = geom(t)
        wait_total((ys - 1) * zs * (rows - a) * half, yrecv.at[t])
        for yy in ypeers:
            rdma(outs[w].at[:, yy, excl, col], outs[w].at[:, yy, excl, col], xsend.at[t], xrecv.at[t], (par, s))
            rdma(outs[w].at[:, yy, mine, col], outs[w].at[:, yy, mine, col], csend.at[t], crecv.at[t], (sib, s))

    def stage_c(t):
        w, a, half, rows, mine, excl, missing, col = geom(t)
        wait_total((zs * ys - 1) * a * half, xrecv.at[t])
        for zz in zpeers:
            rdma(outs[w].at[zz, y, missing, col], outs[w].at[zz, y, missing, col], csend.at[t], crecv.at[t], (sib, s))
        for yy in ypeers:
            rdma(outs[w].at[:, yy, missing, col], outs[w].at[:, yy, missing, col], csend.at[t], crecv.at[t], (sib, s))

    n = len(chunks)
    for t in range(n):
        stage_z(t)
    for cp in local:
        cp.wait()
    for t in range(n + 2):
        if t < n:
            stage_y(t)
        if 0 <= t - 1 < n:
            stage_x(t - 1)
        if 0 <= t - 2 < n:
            stage_c(t - 2)
    for t in range(n):
        w, a, half, rows, mine, excl, missing, col = geom(t)
        wait_total((zs * ys - 1) * rows * half, crecv.at[t])
        wait_total((zs * ys - 1) * rows * half, csend.at[t])
        wait_total((zs * ys - 1) * a * half, xsend.at[t])
        wait_total((zs - 1) * (rows - a) * half, zsend.at[t])
        wait_total((ys - 1) * zs * (rows - a) * half, ysend.at[t])


def gather_all(shards, n_rep, n_shard, width=1024, cid=0):
    zs, ys = mesh_split(n_rep, n_shard)
    chunks = chunk_list([w.shape for w in shards], width)
    n = len(chunks)
    nw = len(shards)
    res = pl.pallas_call(
        functools.partial(gather_kernel, nw, zs, ys, chunks),
        out_shape=[jax.ShapeDtypeStruct((zs, ys) + w.shape, w.dtype) for w in shards],
        in_specs=[pl.BlockSpec(memory_space=pltpu.VMEM)] * nw,
        out_specs=[pl.BlockSpec(memory_space=pl.ANY)] * nw,
        scratch_shapes=[pltpu.SemaphoreType.DMA((n,))] * 8 + [pltpu.SemaphoreType.DMA((nw,))],
        compiler_params=pltpu.CompilerParams(collective_id=cid, has_side_effects=True),
        name="gather_weights",
    )(*shards)
    return [v.reshape((-1, v.shape[-1])) for v in res]


def shards(
    inputs,
    cotangent,
    lengths,
    adapter_ids,
    gain_one,
    gain_two,
    qkv_weight,
    out_weight,
    up_weight,
    down_weight,
    adapter_down,
    adapter_up,
):
    gathered = gather_all(
        (qkv_weight, out_weight, up_weight, down_weight, adapter_down, adapter_up),
        lax.axis_size("rep"),
        lax.axis_size("shard"),
    )

    def forward_step(carry, slot):
        tokens, length, adapter = slot
        output, saved = forward_slot(tokens, length, adapter, gathered, gain_one, gain_two)
        return (carry, (output, saved))

    outputs_saved = lax.scan(forward_step, None, (inputs, lengths, adapter_ids))[1]
    outputs, saved_all = outputs_saved
    def backward_step(carry, slot):
        tokens, slot_cot, length, adapter, saved = slot
        grad_input, block_down, block_up = backward_slot(
            tokens, slot_cot, length, adapter, saved, gathered, gain_one, gain_two
        )
        return (carry, (grad_input, block_down, block_up))

    grads, down_blocks, up_blocks = lax.scan(
        backward_step, None, (inputs, cotangent, lengths, adapter_ids, saved_all)
    )[1]
    accum_down = place_blocks(down_blocks, adapter_ids)
    accum_up = place_blocks(up_blocks, adapter_ids)
    owned = (
        lax.psum_scatter(accum_down, "shard", scatter_dimension=0, tiled=True),
        lax.psum_scatter(accum_up, "shard", scatter_dimension=0, tiled=True),
    )
    summed = lax.psum((owned[0], owned[1]), "rep")
    return (outputs, grads, summed[0], summed[1])


def solution(mesh):
    return jax.shard_map(
        shards,
        mesh=mesh,
        in_specs=(
            P(("rep", "shard"), None, None),
            P(("rep", "shard"), None, None),
            P(("rep", "shard")),
            P(("rep", "shard")),
            P(),
            P(),
            P("shard", None),
            P("shard", None),
            P("shard", None),
            P("shard", None),
            P("shard", None),
            P("shard", None),
        ),
        out_specs=(
            P(("rep", "shard"), None, None),
            P(("rep", "shard"), None, None),
            P("shard", None),
            P("shard", None),
        ),
        check_vma=False,
    )
```

```python
import functools

import jax
import jax.numpy as jnp
from jax import lax
from jax.experimental import pallas as pl
from jax.experimental.pallas import tpu as pltpu
from jax.sharding import PartitionSpec as P

MESH = pl.DeviceIdType.MESH

def mesh_split(n_rep, n_shard):
    zs = 4 if n_shard % 4 == 0 else n_shard
    return zs, n_shard // zs

def share_rows(rows):
    return max(16, rows * 3 // 8 // 16 * 16)

def chunk_list(shapes, width):
    out = []
    for w, (rows, cols) in enumerate(shapes):
        for r0 in range(0, rows, 128):
            for c0 in range(0, cols, width):
                out.append((w, r0, min(rows, 128), c0, min(width, cols)))
    return out

def gather_kernel(n_w, zs, ys, chunks, *refs):
    ins = refs[:n_w]
    outs = refs[n_w:2 * n_w]
    zsend, zrecv, ysend, yrecv, xsend, xrecv, csend, crecv, lsem = refs[2 * n_w:]
    r = lax.axis_index("rep")
    s = lax.axis_index("shard")
    z, y = s // ys, lax.rem(s, ys)
    core = lax.rem(r, 2)
    xp = lax.rem(r // 2, 2)
    sib = r + 1 - 2 * core
    par = r + 2 - 4 * xp
    zpeers = [lax.rem(z + k, zs) for k in range(1, zs)]
    ypeers = [lax.rem(y + k, ys) for k in range(1, ys)]
    peers = [(r, zz * ys + y) for zz in zpeers] + [(r, z * ys + yy) for yy in ypeers] + [(par, s), (sib, s)]
    local = []
    for w in range(n_w):
        cp = pltpu.make_async_copy(ins[w], outs[w].at[z, y], lsem.at[w])
        cp.start()
        local.append(cp)
    bar = pltpu.get_barrier_semaphore()
    for p in peers:
        pl.semaphore_signal(bar, inc=1, device_id=p, device_id_type=MESH)
    pl.semaphore_wait(bar, len(peers))

    def rdma(src, dst, ss, rs, dev):
        cp = pltpu.make_async_remote_copy(src_ref=src, dst_ref=dst, send_sem=ss, recv_sem=rs, device_id=dev, device_id_type=MESH)
        cp.start()

    def geom(t):
        w, r0, rows, c0, cols = chunks[t]
        a = share_rows(rows)
        half = cols // 2
        mine = pl.ds(pl.multiple_of(r0 + xp * a, 16), rows - a)
        excl = pl.ds(pl.multiple_of(r0 + xp * (rows - a), 16), a)
        missing = pl.ds(pl.multiple_of(r0 + (1 - xp) * (rows - a), 16), a)
        col = pl.ds(pl.multiple_of(c0 + core * half, 128), half)
        return w, a, half, rows, mine, excl, missing, col

    def wait_total(elems, sem):
        for out in outs:
            _, _, big_r, big_n = out.shape
            for lead in range(1, zs + 1):
                for take in range(big_r, 0, -16):
                    if elems % (lead * take * 128) == 0 and elems // (lead * take) <= big_n:
                        reg = out.at[pl.ds(0, lead), 0, pl.ds(0, take), pl.ds(0, elems // (lead * take))]
                        pltpu.make_async_copy(reg, reg, sem).wait()
                        return
        raise ValueError("no region")

    def stage_z(t):
        w, a, half, rows, mine, excl, missing, col = geom(t)
        for zz in zpeers:
            rdma(ins[w].at[mine, col], outs[w].at[z, y, mine, col], zsend.at[t], zrecv.at[t], (r, zz * ys + y))

    def stage_y(t):
        w, a, half, rows, mine, excl, missing, col = geom(t)
        wait_total((zs - 1) * (rows - a) * half, zrecv.at[t])
        for yy in ypeers:
            rdma(outs[w].at[:, y, mine, col], outs[w].at[:, y, mine, col], ysend.at[t], yrecv.at[t], (r, z * ys + yy))
        for zz in zpeers:
            rdma(outs[w].at[zz, y, excl, col], outs[w].at[zz, y, excl, col], xsend.at[t], xrecv.at[t], (par, s))
            rdma(outs[w].at[zz, y, mine, col], outs[w].at[zz, y, mine, col], csend.at[t], crecv.at[t], (sib, s))

    def stage_x(t):
        w, a, half, rows, mine, excl, missing, col = geom(t)
        wait_total((ys - 1) * zs * (rows - a) * half, yrecv.at[t])
        for yy in ypeers:
            rdma(outs[w].at[:, yy, excl, col], outs[w].at[:, yy, excl, col], xsend.at[t], xrecv.at[t], (par, s))
            rdma(outs[w].at[:, yy, mine, col], outs[w].at[:, yy, mine, col], csend.at[t], crecv.at[t], (sib, s))

    def stage_c(t):
        w, a, half, rows, mine, excl, missing, col = geom(t)
        wait_total((zs * ys - 1) * a * half, xrecv.at[t])
        for zz in zpeers:
            rdma(outs[w].at[zz, y, missing, col], outs[w].at[zz, y, missing, col], csend.at[t], crecv.at[t], (sib, s))
        for yy in ypeers:
            rdma(outs[w].at[:, yy, missing, col], outs[w].at[:, yy, missing, col], csend.at[t], crecv.at[t], (sib, s))

    n = len(chunks)
    for t in range(n):
        stage_z(t)
    for cp in local:
        cp.wait()
    for t in range(n + 2):
        if t < n:
            stage_y(t)
        if 0 <= t - 1 < n:
            stage_x(t - 1)
        if 0 <= t - 2 < n:
            stage_c(t - 2)
    for t in range(n):
        w, a, half, rows, mine, excl, missing, col = geom(t)
        wait_total((zs * ys - 1) * rows * half, crecv.at[t])
        wait_total((zs * ys - 1) * rows * half, csend.at[t])
        wait_total((zs * ys - 1) * a * half, xsend.at[t])
        wait_total((zs - 1) * (rows - a) * half, zsend.at[t])
        wait_total((ys - 1) * zs * (rows - a) * half, ysend.at[t])


def gather_all(shards, n_rep, n_shard, width=1024, cid=0):
    zs, ys = mesh_split(n_rep, n_shard)
    chunks = chunk_list([w.shape for w in shards], width)
    n = len(chunks)
    nw = len(shards)
    res = pl.pallas_call(
        functools.partial(gather_kernel, nw, zs, ys, chunks),
        out_shape=[jax.ShapeDtypeStruct((zs, ys) + w.shape, w.dtype) for w in shards],
        in_specs=[pl.BlockSpec(memory_space=pltpu.VMEM)] * nw,
        out_specs=[pl.BlockSpec(memory_space=pl.ANY)] * nw,
        scratch_shapes=[pltpu.SemaphoreType.DMA((n,))] * 8 + [pltpu.SemaphoreType.DMA((nw,))],
        compiler_params=pltpu.CompilerParams(collective_id=cid, has_side_effects=True),
        name="gather_weights",
    )(*shards)
    return [v.reshape((-1, v.shape[-1])) for v in res]


EPS = 1e-05
HEAD = 64
RANK = 16
ADAPTERS = 8
COLS = 4 * RANK
VMEM_CAP = 60 * 1024 * 1024
BF = jnp.bfloat16
F32 = jnp.float32


def dense(left, right):
    return jnp.dot(left, right, preferred_element_type=F32)


def dense_trans(left, right):
    return lax.dot_general(left, right, (((1,), (1,)), ((), ())), preferred_element_type=F32)


def dense_left(left, right):
    return lax.dot_general(left, right, (((0,), (0,)), ((), ())), preferred_element_type=F32)


def lane_group(values, size, group):
    lanes = lax.broadcasted_iota(jnp.int32, values.shape, 1)
    return jnp.where(lanes // size == group, values, jnp.zeros_like(values))


def norm_stats(values):
    center = values - jnp.mean(values, axis=-1, keepdims=True)
    rs = lax.rsqrt(jnp.mean(center * center, axis=-1, keepdims=True) + EPS)
    return center * rs, rs


def norm_back(unit, rs, gain, grad):
    eg = grad * gain
    return rs * (eg - jnp.mean(eg, axis=-1, keepdims=True) - unit * jnp.mean(eg * unit, axis=-1, keepdims=True))


def qkv_body(per_third, x_ref, g_ref, w_ref, down_ref, up_ref, normed_ref, inner_ref, out_ref):
    step = pl.program_id(0)
    rows = 256

    @pl.when(step == 0)
    def _():
        for i in range(x_ref.shape[0] // rows):
            sl = pl.ds(i * rows, rows)
            unit, _ = norm_stats(x_ref[sl, :].astype(F32))
            normed_ref[sl, :] = (unit * g_ref[...]).astype(BF)
            inner_ref[sl, :] = dense(normed_ref[sl, :], down_ref[...]).astype(BF)

    inner = lane_group(inner_ref[...], RANK, step // per_third)
    out_ref[...] = (dense(normed_ref[...], w_ref[...]) + dense_trans(inner, up_ref[...])).astype(BF)


def qkv_forward(x, gain, qkv, down, up):
    seq, dim = x.shape
    total = qkv.shape[1]
    block = min(512, dim)
    per_third = dim // block
    return pl.pallas_call(
        functools.partial(qkv_body, per_third),
        grid=(total // block,),
        out_shape=[
            jax.ShapeDtypeStruct((seq, dim), BF),
            jax.ShapeDtypeStruct((seq, COLS), BF),
            jax.ShapeDtypeStruct((seq, total), BF),
        ],
        in_specs=[
            pl.BlockSpec((seq, dim), lambda j: (0, 0), pipeline_mode=pl.Buffered(1)),
            pl.BlockSpec((1, dim), lambda j: (0, 0)),
            pl.BlockSpec((dim, block), lambda j: (0, j)),
            pl.BlockSpec((dim, COLS), lambda j: (0, 0)),
            pl.BlockSpec((block, COLS), lambda j: (lax.rem(j, per_third), 0)),
        ],
        out_specs=[
            pl.BlockSpec((seq, dim), lambda j: (0, 0)),
            pl.BlockSpec((seq, COLS), lambda j: (0, 0)),
            pl.BlockSpec((seq, block), lambda j: (0, j)),
        ],
        compiler_params=pltpu.CompilerParams(vmem_limit_bytes=VMEM_CAP),
        name="qkv_forward",
    )(x, gain, qkv, down, up)


def attn_fwd_body(tile, q_ref, k_ref, v_ref, ctx_ref, p_ref):
    seq, lanes = q_ref.shape
    heads = lanes // HEAD
    scale = HEAD ** (-0.5)
    rows = lax.broadcasted_iota(jnp.int32, (tile, tile), 0)
    cols = lax.broadcasted_iota(jnp.int32, (tile, tile), 1)
    keep = rows >= cols
    off = 0
    for i in range(seq // tile):
        stop = (i + 1) * tile
        q = q_ref[pl.ds(i * tile, tile), :] * jnp.asarray(scale, BF)
        acc = None
        for h in range(heads):
            qh = lane_group(q, HEAD, h)
            s = dense_trans(qh, k_ref[pl.ds(0, stop), :])
            diag = jnp.where(keep, s[:, stop - tile :], -1e30)
            s = diag if i == 0 else jnp.concatenate([s[:, : stop - tile], diag], axis=1)
            peak = jnp.max(s, axis=-1, keepdims=True)
            e = jnp.exp(s - peak)
            inv = 1.0 / jnp.sum(e, axis=-1, keepdims=True)
            p = (e * inv).astype(BF)
            p_ref[h, :, pl.ds(off, stop)] = p
            o = dense(p, lane_group(v_ref[pl.ds(0, stop), :], HEAD, h))
            acc = o if acc is None else acc + o
        ctx_ref[pl.ds(i * tile, tile), :] = acc.astype(BF)
        off += stop


def attention_forward(proj, tile, lanes=128):
    seq = proj.shape[0]
    width = proj.shape[1] // 3
    n = width // lanes
    heads = lanes // HEAD
    packed = tile * (seq // tile) * (seq // tile + 1) // 2
    return pl.pallas_call(
        functools.partial(attn_fwd_body, tile),
        grid=(n,),
        out_shape=[
            jax.ShapeDtypeStruct((seq, width), BF),
            jax.ShapeDtypeStruct((width // HEAD, tile, packed), BF),
        ],
        in_specs=[pl.BlockSpec((seq, lanes), lambda j, t=t: (0, t * n + j)) for t in range(3)],
        out_specs=[
            pl.BlockSpec((seq, lanes), lambda j: (0, j)),
            pl.BlockSpec((heads, tile, packed), lambda j: (j, 0, 0)),
        ],
        compiler_params=pltpu.CompilerParams(vmem_limit_bytes=VMEM_CAP),
        name="attention_forward",
    )(proj, proj, proj)


def attn_bwd_body(tile, q_ref, k_ref, v_ref, go_ref, ctx_ref, p_ref, dq_ref, dk_ref, dv_ref, dk_acc, dv_acc):
    seq, lanes = q_ref.shape
    heads = lanes // HEAD
    scale = HEAD ** (-0.5)
    off = 0
    n = seq // tile
    dk_acc[...] = jnp.zeros_like(dk_acc)
    dv_acc[...] = jnp.zeros_like(dv_acc)
    for i in range(n):
        stop = (i + 1) * tile
        sl = pl.ds(i * tile, tile)
        past = pl.ds(0, stop)
        go = go_ref[sl, :]
        q = q_ref[sl, :]
        prod = go.astype(F32) * ctx_ref[sl, :].astype(F32)
        acc = None
        for h in range(heads):
            delta = jnp.sum(lane_group(prod, HEAD, h), axis=-1, keepdims=True)
            gh = lane_group(go, HEAD, h)
            p = p_ref[h, :, pl.ds(off, stop)]
            dp = dense_trans(gh, v_ref[past, :])
            ds = (p.astype(F32) * (dp - delta)).astype(BF)
            dv_acc[past, :] += dense_left(p, gh)
            dk_acc[past, :] += dense_left(ds, lane_group(q, HEAD, h))
            o = dense(ds, lane_group(k_ref[past, :], HEAD, h))
            acc = o if acc is None else acc + o
        dq_ref[sl, :] = (acc * scale).astype(BF)
        off += stop
    dk_ref[...] = (dk_acc[...] * scale).astype(BF)
    dv_ref[...] = dv_acc[...].astype(BF)


def attention_backward(proj, grad_ctx, ctx, probs, tile, lanes=128):
    seq = proj.shape[0]
    width = proj.shape[1] // 3
    n = width // lanes
    heads = lanes // HEAD
    packed = probs.shape[2]
    blk = pl.BlockSpec((seq, lanes), lambda j: (0, j))
    return pl.pallas_call(
        functools.partial(attn_bwd_body, tile),
        grid=(n,),
        out_shape=[jax.ShapeDtypeStruct((seq, width), BF)] * 3,
        in_specs=[pl.BlockSpec((seq, lanes), lambda j, t=t: (0, t * n + j)) for t in range(3)]
        + [blk, blk, pl.BlockSpec((heads, tile, packed), lambda j: (j, 0, 0))],
        out_specs=[blk] * 3,
        scratch_shapes=[pltpu.VMEM((seq, lanes), F32)] * 2,
        compiler_params=pltpu.CompilerParams(vmem_limit_bytes=VMEM_CAP),
        name="attention_backward",
    )(proj, proj, proj, grad_ctx, ctx, probs)


def mlp_body(
    chunk, len_ref, x_ref, ctx_ref, cot_ref, g_ref, out_w, up_w, down_w, adn_ref, aup_ref,
    y_ref, gh_ref, gc_ref, dgrad_ref, ugrad_ref, nt_ref, mlp_acc, gn_acc,
):
    step = pl.program_id(0)
    rows = x_ref.shape[0]
    ctx = ctx_ref[...]
    inner_out = lane_group(dense(ctx, adn_ref[...]), RANK, 3).astype(BF)
    hidden = x_ref[...].astype(F32) + (dense(ctx, out_w[...]) + dense_trans(inner_out, aup_ref[...]))
    unit, rs = norm_stats(hidden)
    nt_ref[...] = (unit * g_ref[...]).astype(BF)
    pos = step * rows + lax.broadcasted_iota(jnp.int32, (rows, 1), 0)
    valid = pos < len_ref[0]
    cot = cot_ref[...]
    grad_mlp = jnp.where(valid, cot, jnp.zeros_like(cot))
    ff = up_w.shape[1]
    mlp_acc[...] = jnp.zeros_like(mlp_acc)
    gn_acc[...] = jnp.zeros_like(gn_acc)

    def one(f, carry):
        fs = pl.ds(pl.multiple_of(f * chunk, chunk), chunk)
        u = dense(nt_ref[...], up_w[:, fs])
        ga = dense_trans(grad_mlp, down_w[fs, :])
        k = 0.7978845608028654
        sq = u * u
        t = jnp.tanh(k * (u + 0.044715 * u * sq))
        half = 0.5 * (1.0 + t)
        act = (u * half).astype(BF)
        d = half + 0.5 * u * (1.0 - t * t) * (k * (1.0 + (3.0 * 0.044715) * sq))
        gp = (ga * d).astype(BF)
        mlp_acc[...] += dense(act, down_w[fs, :])
        gn_acc[...] += dense_trans(gp, up_w[:, fs])
        return carry

    lax.fori_loop(0, ff // chunk, one, 0, unroll=2)
    y_ref[...] = jnp.where(valid, hidden + mlp_acc[...], 0.0).astype(BF)
    gh = grad_mlp.astype(F32) + norm_back(unit, rs, g_ref[...], gn_acc[...])
    gh_ref[...] = gh
    ga = gh.astype(BF)
    gio = lane_group(dense(ga, aup_ref[...]), RANK, 3).astype(BF)
    gc_ref[...] = (dense_trans(ga, out_w[...]) + dense_trans(gio, adn_ref[...])).astype(BF)

    @pl.when(step == 0)
    def _():
        dgrad_ref[...] = jnp.zeros_like(dgrad_ref)
        ugrad_ref[...] = jnp.zeros_like(ugrad_ref)

    dgrad_ref[...] += dense_left(gio, ctx)
    ugrad_ref[...] += dense_left(inner_out, ga)


def mlp_both(length, x, ctx, cot, gain, out_w, up_w, down_w, adn, aup, rows=256, chunk=512):
    seq, dim = x.shape
    ff = up_w.shape[1]
    row = pl.BlockSpec((rows, dim), lambda i: (i, 0))

    def whole(shape):
        return pl.BlockSpec(shape, lambda i: (0, 0), pipeline_mode=pl.Buffered(1))

    return pl.pallas_call(
        functools.partial(mlp_body, chunk),
        grid=(seq // rows,),
        out_shape=[
            jax.ShapeDtypeStruct((seq, dim), BF),
            jax.ShapeDtypeStruct((seq, dim), F32),
            jax.ShapeDtypeStruct((seq, dim), BF),
            jax.ShapeDtypeStruct((COLS, dim), F32),
            jax.ShapeDtypeStruct((COLS, dim), F32),
        ],
        in_specs=[
            pl.BlockSpec(memory_space=pltpu.SMEM),
            row, row, row,
            whole((1, dim)), whole((dim, dim)), whole((dim, ff)), whole((ff, dim)), whole((dim, COLS)), whole((dim, COLS)),
        ],
        out_specs=[row, row, row, whole((COLS, dim)), whole((COLS, dim))],
        scratch_shapes=[pltpu.VMEM((rows, dim), BF), pltpu.VMEM((rows, dim), F32), pltpu.VMEM((rows, dim), F32)],
        compiler_params=pltpu.CompilerParams(vmem_limit_bytes=VMEM_CAP),
        name="mlp_forward_backward",
    )(length, x, ctx, cot, gain, out_w, up_w, down_w, adn, aup)


def tail_body(
    x_ref, gh_ref, normed_ref, inner_ref, dq_ref, dk_ref, dv_ref, g_ref, w_ref, adn_ref, aup_ref, din_ref, uin_ref,
    id_ref, gx_ref, pay_ref, dgrad_ref, ugrad_ref,
):
    step = pl.program_id(0)
    dim = x_ref.shape[1]
    thirds = [dq_ref[...], dk_ref[...], dv_ref[...]]
    gi = None
    gn = None
    for p in range(3):
        one = lane_group(dense(thirds[p], aup_ref[...]), RANK, p)
        gi = one if gi is None else gi + one
        g = dense_trans(thirds[p], w_ref[:, pl.ds(p * dim, dim)])
        gn = g if gn is None else gn + g
    gi = gi.astype(BF)
    gn = gn + dense_trans(gi, adn_ref[...])
    unit, rs = norm_stats(x_ref[...].astype(F32))
    gx_ref[...] = (gh_ref[...] + norm_back(unit, rs, g_ref[...], gn)).astype(BF)

    @pl.when(step == 0)
    def _():
        dgrad_ref[...] = din_ref[...]
        ugrad_ref[...] = uin_ref[...]

    dgrad_ref[...] += dense_left(gi, normed_ref[...])
    up = None
    for p in range(3):
        one = dense_left(lane_group(inner_ref[...], RANK, p), thirds[p])
        up = one if up is None else up + one
    ugrad_ref[...] += up

    @pl.when(step == pl.num_programs(0) - 1)
    def _():
        n, pay, width = pay_ref.shape
        mark = jnp.full((pay - 2 * COLS, width), id_ref[0], jnp.int32).astype(F32)
        for i in range(n):
            sl = pl.ds(i * width, width)
            pay_ref[i] = jnp.concatenate([dgrad_ref[:, sl], ugrad_ref[:, sl], mark], axis=0).astype(BF)


def tail_backward(x, gh, normed, inner, dq, dk, dv, gain, qkv, adn, aup, din, uin, adapter, n_shard, rows=256):
    seq, dim = x.shape
    row = pl.BlockSpec((rows, dim), lambda i: (i, 0))

    def whole(shape):
        return pl.BlockSpec(shape, lambda i: (0, 0), pipeline_mode=pl.Buffered(1))

    return pl.pallas_call(
        tail_body,
        grid=(seq // rows,),
        out_shape=[
            jax.ShapeDtypeStruct((seq, dim), BF),
            jax.ShapeDtypeStruct((n_shard, PAY, dim // n_shard), BF),
        ],
        in_specs=[
            row, row, row, pl.BlockSpec((rows, COLS), lambda i: (i, 0)), row, row, row,
            whole((1, dim)), whole(qkv.shape), whole((dim, COLS)), whole((dim, COLS)), whole((COLS, dim)), whole((COLS, dim)),
            pl.BlockSpec(memory_space=pltpu.SMEM),
        ],
        out_specs=[row, pl.BlockSpec((n_shard, PAY, dim // n_shard), lambda i: (0, 0, 0))],
        scratch_shapes=[pltpu.VMEM((COLS, dim), F32)] * 2,
        compiler_params=pltpu.CompilerParams(vmem_limit_bytes=VMEM_CAP),
        name="tail_backward",
    )(x, gh, normed, inner, dq, dk, dv, gain, qkv, adn, aup, din, uin, adapter)


def one_slot(tokens, slot_cot, length, adapter, weights, gain_one, gain_two, n_shard):
    qkv, out_w, up_w, down_w, adapter_down, adapter_up = weights
    first = adapter * COLS
    adn = lax.dynamic_slice_in_dim(adapter_down, first, COLS, 1)
    aup = lax.dynamic_slice_in_dim(adapter_up, first, COLS, 1)
    tile = 256 if tokens.shape[0] % 256 == 0 else tokens.shape[0]
    g_one, g_two = gain_one[None], gain_two[None]
    normed, inner, proj = qkv_forward(tokens, g_one, qkv, adn, aup)
    ctx, probs = attention_forward(proj, tile)
    y, gh, gc, dg, ug = mlp_both(length, tokens, ctx, slot_cot, g_two, out_w, up_w, down_w, adn, aup)
    dq, dk, dv = attention_backward(proj, gc, ctx, probs, tile)
    gx, pay = tail_backward(
        tokens, gh, normed, inner, dq, dk, dv, g_one, qkv, adn, aup, dg, ug, adapter[None], n_shard
    )
    return y, gx, pay


PAY = 2 * COLS + 16


def flip(value, bit):
    return value + bit - 2 * bit * lax.rem(value // bit, 2)


def reduce_body(n_rep, n_shard, bits, pay_ref, down_ref, up_ref, buf, send, recv, xsend, xrecv, lsem):
    r = lax.axis_index("rep")
    s = lax.axis_index("shard")
    others = [lax.rem(s + k, n_shard) for k in range(1, n_shard)]
    peers = [(r, o) for o in others] + [(flip(r, b), s) for b in bits]
    own = pltpu.make_async_copy(pay_ref.at[s], buf.at[r, s], lsem)
    own.start()
    bar = pltpu.get_barrier_semaphore()
    for p in peers:
        pl.semaphore_signal(bar, inc=1, device_id=p, device_id_type=MESH)
    pl.semaphore_wait(bar, len(peers))
    copies = []
    for k, o in enumerate(others):
        cp = pltpu.make_async_remote_copy(
            src_ref=pay_ref.at[o], dst_ref=buf.at[r, s], send_sem=send.at[k], recv_sem=recv.at[k],
            device_id=(r, o), device_id_type=MESH,
        )
        cp.start()
        copies.append(cp)
    own.wait()
    for cp in copies:
        cp.wait()
    held = [0]
    at = 0
    for b in bits:
        partner = flip(r, b)
        copies = []
        for m in held:
            q = r
            for c in bits:
                if m & c:
                    q = flip(q, c)
            cp = pltpu.make_async_remote_copy(
                src_ref=buf.at[q], dst_ref=buf.at[q], send_sem=xsend.at[at], recv_sem=xrecv.at[at],
                device_id=(partner, s), device_id_type=MESH,
            )
            cp.start()
            copies.append(cp)
            at += 1
        for cp in copies:
            cp.wait()
        held = held + [m | b for m in held]
    rows = buf.shape[3]
    for a in range(ADAPTERS):

        def add(i, acc):
            low = buf[i // n_shard, lax.rem(i, n_shard)]
            block = low[: 2 * COLS, :].astype(F32)
            mark = low[2 * COLS : 2 * COLS + 8, :].astype(F32)[0:1, :]
            return acc + jnp.where(mark == float(a), block, 0.0)

        total = lax.fori_loop(0, n_rep * n_shard, add, jnp.zeros((2 * COLS, rows), F32), unroll=4)
        flat = jnp.transpose(total)
        down_ref[:, pl.ds(a * COLS, COLS)] = flat[:, :COLS]
        up_ref[:, pl.ds(a * COLS, COLS)] = flat[:, COLS:]


def reduce_grads(pay, n_rep, n_shard):
    bits = [1 << k for k in range(1, n_rep.bit_length() - 1)] + [1]
    rows = pay.shape[2]
    return pl.pallas_call(
        functools.partial(reduce_body, n_rep, n_shard, bits),
        out_shape=[jax.ShapeDtypeStruct((rows, ADAPTERS * COLS), F32)] * 2,
        in_specs=[pl.BlockSpec(memory_space=pltpu.VMEM)],
        out_specs=[pl.BlockSpec(memory_space=pltpu.VMEM)] * 2,
        scratch_shapes=[pltpu.VMEM((n_rep, n_shard, PAY, rows), BF)]
        + [pltpu.SemaphoreType.DMA((n_shard - 1,))] * 2
        + [pltpu.SemaphoreType.DMA((n_rep - 1,))] * 2
        + [pltpu.SemaphoreType.DMA],
        compiler_params=pltpu.CompilerParams(collective_id=1, has_side_effects=True, vmem_limit_bytes=VMEM_CAP),
        name="reduce_grads",
    )(pay)


def shards(
    inputs,
    cotangent,
    lengths,
    adapter_ids,
    gain_one,
    gain_two,
    qkv_weight,
    out_weight,
    up_weight,
    down_weight,
    adapter_down,
    adapter_up,
):
    n_rep, n_shard = lax.axis_size("rep"), lax.axis_size("shard")
    weights = gather_all(
        (qkv_weight, out_weight, up_weight, down_weight, adapter_down, adapter_up), n_rep, n_shard
    )
    output, grad, pay = one_slot(
        inputs[0], cotangent[0], lengths, adapter_ids[0], weights, gain_one, gain_two, n_shard
    )
    down_grad, up_grad = reduce_grads(pay, n_rep, n_shard)
    return (output[None], grad[None], down_grad, up_grad)


def solution(mesh):
    return jax.shard_map(
        shards,
        mesh=mesh,
        in_specs=(
            P(("rep", "shard"), None, None),
            P(("rep", "shard"), None, None),
            P(("rep", "shard")),
            P(("rep", "shard")),
            P(),
            P(),
            P("shard", None),
            P("shard", None),
            P("shard", None),
            P("shard", None),
            P("shard", None),
            P("shard", None),
        ),
        out_specs=(
            P(("rep", "shard"), None, None),
            P(("rep", "shard"), None, None),
            P("shard", None),
            P("shard", None),
        ),
        check_vma=False,
    )
```

```python
import functools

import jax
import jax.numpy as jnp
from jax import lax
from jax.experimental import pallas as pl
from jax.experimental.pallas import tpu as pltpu
from jax.sharding import PartitionSpec as P

MESH = pl.DeviceIdType.MESH

def mesh_split(n_rep, n_shard):
    zs = 4 if n_shard % 4 == 0 else n_shard
    return zs, n_shard // zs

def share_rows(rows):
    return max(16, rows * 3 // 8 // 16 * 16)


EPS = 1e-05
HEAD = 64
RANK = 16
ADAPTERS = 8
COLS = 4 * RANK
VMEM_CAP = 60 * 1024 * 1024
BF = jnp.bfloat16
F32 = jnp.float32


def dense(left, right):
    return jnp.dot(left, right, preferred_element_type=F32)


def dense_trans(left, right):
    return lax.dot_general(left, right, (((1,), (1,)), ((), ())), preferred_element_type=F32)


def dense_left(left, right):
    return lax.dot_general(left, right, (((0,), (0,)), ((), ())), preferred_element_type=F32)


def lane_group(values, size, group):
    lanes = lax.broadcasted_iota(jnp.int32, values.shape, 1)
    return jnp.where(lanes // size == group, values, jnp.zeros_like(values))


def norm_stats(values):
    center = values - jnp.mean(values, axis=-1, keepdims=True)
    rs = lax.rsqrt(jnp.mean(center * center, axis=-1, keepdims=True) + EPS)
    return center * rs, rs


def norm_back(unit, rs, gain, grad):
    eg = grad * gain
    return rs * (eg - jnp.mean(eg, axis=-1, keepdims=True) - unit * jnp.mean(eg * unit, axis=-1, keepdims=True))


def attn_fwd_body(tile, q_ref, k_ref, v_ref, ctx_ref, p_ref):
    seq, lanes = q_ref.shape
    heads = lanes // HEAD
    scale = HEAD ** (-0.5)
    rows = lax.broadcasted_iota(jnp.int32, (tile, tile), 0)
    cols = lax.broadcasted_iota(jnp.int32, (tile, tile), 1)
    keep = rows >= cols
    off = 0
    for i in range(seq // tile):
        stop = (i + 1) * tile
        q = q_ref[pl.ds(i * tile, tile), :] * jnp.asarray(scale, BF)
        acc = None
        for h in range(heads):
            qh = lane_group(q, HEAD, h)
            s = dense_trans(qh, k_ref[pl.ds(0, stop), :])
            diag = jnp.where(keep, s[:, stop - tile :], -1e30)
            s = diag if i == 0 else jnp.concatenate([s[:, : stop - tile], diag], axis=1)
            peak = jnp.max(s, axis=-1, keepdims=True)
            e = jnp.exp(s - peak)
            inv = 1.0 / jnp.sum(e, axis=-1, keepdims=True)
            p = (e * inv).astype(BF)
            p_ref[h, :, pl.ds(off, stop)] = p
            o = dense(p, lane_group(v_ref[pl.ds(0, stop), :], HEAD, h))
            acc = o if acc is None else acc + o
        ctx_ref[pl.ds(i * tile, tile), :] = acc.astype(BF)
        off += stop


def attn_bwd_body(tile, q_ref, k_ref, v_ref, go_ref, ctx_ref, p_ref, dq_ref, dk_ref, dv_ref, dk_acc, dv_acc):
    seq, lanes = q_ref.shape
    heads = lanes // HEAD
    scale = HEAD ** (-0.5)
    off = 0
    n = seq // tile
    dk_acc[...] = jnp.zeros_like(dk_acc)
    dv_acc[...] = jnp.zeros_like(dv_acc)
    for i in range(n):
        stop = (i + 1) * tile
        sl = pl.ds(i * tile, tile)
        past = pl.ds(0, stop)
        go = go_ref[sl, :]
        q = q_ref[sl, :]
        prod = go.astype(F32) * ctx_ref[sl, :].astype(F32)
        acc = None
        for h in range(heads):
            delta = jnp.sum(lane_group(prod, HEAD, h), axis=-1, keepdims=True)
            gh = lane_group(go, HEAD, h)
            p = p_ref[h, :, pl.ds(off, stop)]
            dp = dense_trans(gh, v_ref[past, :])
            ds = (p.astype(F32) * (dp - delta)).astype(BF)
            dv_acc[past, :] += dense_left(p, gh)
            dk_acc[past, :] += dense_left(ds, lane_group(q, HEAD, h))
            o = dense(ds, lane_group(k_ref[past, :], HEAD, h))
            acc = o if acc is None else acc + o
        dq_ref[sl, :] = (acc * scale).astype(BF)
        off += stop
    dk_ref[...] = (dk_acc[...] * scale).astype(BF)
    dv_ref[...] = dv_acc[...].astype(BF)


def attention_backward(proj, grad_ctx, ctx, probs, tile, lanes=128):
    seq = proj.shape[0]
    width = proj.shape[1] // 3
    n = width // lanes
    heads = lanes // HEAD
    packed = probs.shape[2]
    blk = pl.BlockSpec((seq, lanes), lambda j: (0, j))
    return pl.pallas_call(
        functools.partial(attn_bwd_body, tile),
        grid=(n,),
        out_shape=[jax.ShapeDtypeStruct((seq, width), BF)] * 3,
        in_specs=[pl.BlockSpec((seq, lanes), lambda j, t=t: (0, t * n + j)) for t in range(3)]
        + [blk, blk, pl.BlockSpec((heads, tile, packed), lambda j: (j, 0, 0))],
        out_specs=[blk] * 3,
        scratch_shapes=[pltpu.VMEM((seq, lanes), F32)] * 2,
        compiler_params=pltpu.CompilerParams(vmem_limit_bytes=VMEM_CAP),
        name="attention_backward",
    )(proj, proj, proj, grad_ctx, ctx, probs)


def tail_body(
    x_ref, gh_ref, inner_ref, dq_ref, dk_ref, dv_ref, g_ref, w_ref, adn_ref, aup_ref, din_ref, uin_ref,
    id_ref, gx_ref, pay_ref, dgrad_ref, ugrad_ref,
):
    step = pl.program_id(0)
    dim = x_ref.shape[1]
    thirds = [dq_ref[...], dk_ref[...], dv_ref[...]]
    gi = None
    gn = None
    for p in range(3):
        one = lane_group(dense(thirds[p], aup_ref[...]), RANK, p)
        gi = one if gi is None else gi + one
        g = dense_trans(thirds[p], w_ref[:, pl.ds(p * dim, dim)])
        gn = g if gn is None else gn + g
    gi = gi.astype(BF)
    gn = gn + dense_trans(gi, adn_ref[...])
    unit, rs = norm_stats(x_ref[...].astype(F32))
    normed = (unit * g_ref[...]).astype(BF)
    gx_ref[...] = (gh_ref[...] + norm_back(unit, rs, g_ref[...], gn)).astype(BF)

    @pl.when(step == 0)
    def _():
        dgrad_ref[...] = din_ref[...]
        ugrad_ref[...] = uin_ref[...]

    dgrad_ref[...] += dense_left(gi, normed)
    up = None
    for p in range(3):
        one = dense_left(lane_group(inner_ref[...], RANK, p), thirds[p])
        up = one if up is None else up + one
    ugrad_ref[...] += up

    @pl.when(step == pl.num_programs(0) - 1)
    def _():
        n, pay, width = pay_ref.shape
        mark = jnp.full((pay - 2 * COLS, width), id_ref[0], jnp.int32).astype(F32)
        for i in range(n):
            sl = pl.ds(i * width, width)
            pay_ref[i] = jnp.concatenate([dgrad_ref[:, sl], ugrad_ref[:, sl], mark], axis=0).astype(BF)


def tail_backward(x, gh, inner, dq, dk, dv, gain, qkv, adn, aup, din, uin, adapter, n_shard, rows=256):
    seq, dim = x.shape
    row = pl.BlockSpec((rows, dim), lambda i: (i, 0))

    def whole(shape):
        return pl.BlockSpec(shape, lambda i: (0, 0), pipeline_mode=pl.Buffered(1))

    return pl.pallas_call(
        tail_body,
        grid=(seq // rows,),
        out_shape=[
            jax.ShapeDtypeStruct((seq, dim), BF),
            jax.ShapeDtypeStruct((n_shard, PAY, dim // n_shard), BF),
        ],
        in_specs=[
            row, row, pl.BlockSpec((rows, COLS), lambda i: (i, 0)), row, row, row,
            whole((1, dim)), whole(qkv.shape), whole((dim, COLS)), whole((dim, COLS)), whole((COLS, dim)), whole((COLS, dim)),
            pl.BlockSpec(memory_space=pltpu.SMEM),
        ],
        out_specs=[row, pl.BlockSpec((n_shard, PAY, dim // n_shard), lambda i: (0, 0, 0))],
        scratch_shapes=[pltpu.VMEM((COLS, dim), F32)] * 2,
        compiler_params=pltpu.CompilerParams(vmem_limit_bytes=VMEM_CAP),
        name="tail_backward",
    )(x, gh, inner, dq, dk, dv, gain, qkv, adn, aup, din, uin, adapter)


class Mover:
    def __init__(self, zs, ys, shards, lands, sems, chunks, ahead):
        self.ahead = ahead
        self.zs, self.ys, self.shards, self.lands, self.sems, self.chunks = zs, ys, shards, lands, sems, chunks
        self.r = lax.axis_index("rep")
        self.s = lax.axis_index("shard")
        self.z, self.y = self.s // ys, lax.rem(self.s, ys)
        self.core = lax.rem(self.r, 2)
        self.xp = lax.rem(self.r // 2, 2)
        self.sib = (self.r + 1 - 2 * self.core, self.s)
        self.par = (self.r + 2 - 4 * self.xp, self.s)
        self.ypeers = [lax.rem(self.y + k, ys) for k in range(1, ys)]

    def at_z(self, off):
        return lax.rem(self.z + off, self.zs)

    def barrier(self):
        peers = [(self.r, self.at_z(k) * self.ys + self.y) for k in range(1, self.zs)]
        peers += [(self.r, self.z * self.ys + v) for v in self.ypeers] + [self.par, self.sib]
        bar = pltpu.get_barrier_semaphore()
        for p in peers:
            pl.semaphore_signal(bar, inc=1, device_id=p, device_id_type=MESH)
        pl.semaphore_wait(bar, len(peers))

    def geom(self, t, dest_z):
        w, offs, rows, c0, cols, turn = self.chunks[t]
        a = share_rows(rows)
        half = cols // 2
        mine = pl.ds(pl.multiple_of(self.xp * a, 16), rows - a)
        excl = pl.ds(pl.multiple_of(self.xp * (rows - a), 16), a)
        missing = pl.ds(pl.multiple_of((1 - self.xp) * (rows - a), 16), a)
        first = c0 + self.core * half
        if turn is not None:
            k, span = turn
            first = first + lax.rem(dest_z + k, self.zs) * span
        return w, offs, rows, a, half, mine, excl, missing, pl.ds(pl.multiple_of(first, 128), half)

    def send(self, src, w, zz, yy, rows, col, t, stage, device):
        pltpu.make_async_remote_copy(
            src_ref=src, dst_ref=self.lands[w].at[zz, yy, rows, col], send_sem=self.sems[2 * stage].at[t],
            recv_sem=self.sems[2 * stage + 1].at[t], device_id=device, device_id_type=MESH,
        ).start()

    def relay(self, w, zz, yy, rows, col, t, stage, device):
        self.send(self.lands[w].at[zz, yy, rows, col], w, zz, yy, rows, col, t, stage, device)

    def wait(self, t, stage, side):
        w, offs, rows, a, half, *_ = self.geom(t, self.z)
        far = len([o for o in offs if o])
        near = len(offs) * (self.ys - 1)
        count = ((far * (rows - a)), near * (rows - a), (far + near) * a, (far + near) * rows)[stage]
        if count == 0:
            return
        sem = self.sems[2 * stage + side].at[t]
        elems = count * half
        for out in self.lands:
            _, _, big_r, big_n = out.shape
            for lead in range(1, self.zs + 1):
                for take in range(big_r, 0, -16):
                    if elems % (lead * take * 128) == 0 and elems // (lead * take) <= big_n:
                        reg = out.at[pl.ds(0, lead), 0, pl.ds(0, take), pl.ds(0, elems // (lead * take))]
                        pltpu.make_async_copy(reg, reg, sem).wait()
                        return
        raise ValueError("no region")

    def start_z(self, t):
        offs = self.chunks[t][1]
        for k in range(1, self.zs):
            if (self.zs - k) % self.zs in offs:
                zz = self.at_z(k)
                w, _, _, _, _, mine, _, _, col = self.geom(t, zz)
                self.send(self.shards[w].at[mine, col], w, self.z, self.y, mine, col, t, 0, (self.r, zz * self.ys + self.y))

    def start_y(self, t):
        w, offs, _, _, _, mine, _, _, col = self.geom(t, self.z)
        if 0 in offs:
            for v in self.ypeers:
                self.send(self.shards[w].at[mine, col], w, self.z, self.y, mine, col, t, 1, (self.r, self.z * self.ys + v))

    def begin(self):
        for t in range(min(self.ahead, len(self.chunks))):
            self.start_z(t)
            self.start_y(t)

    def relay_z(self, m):
        if m + self.ahead < len(self.chunks):
            self.start_z(m + self.ahead)
            self.start_y(m + self.ahead)
        w, offs, rows, a, half, mine, excl, missing, col = self.geom(m, self.z)
        self.wait(m, 0, 1)
        for o in offs:
            if o:
                for v in self.ypeers:
                    self.relay(w, self.at_z(o), self.y, mine, col, m, 1, (self.r, self.z * self.ys + v))
        for o in offs:
            if o:
                self.relay(w, self.at_z(o), self.y, excl, col, m, 2, self.par)
                self.relay(w, self.at_z(o), self.y, mine, col, m, 3, self.sib)

    def relay_y(self, m):
        w, offs, rows, a, half, mine, excl, missing, col = self.geom(m, self.z)
        self.wait(m, 1, 1)
        for o in offs:
            for v in self.ypeers:
                self.relay(w, self.at_z(o), v, excl, col, m, 2, self.par)
                self.relay(w, self.at_z(o), v, mine, col, m, 3, self.sib)

    def relay_x(self, m):
        w, offs, rows, a, half, mine, excl, missing, col = self.geom(m, self.z)
        self.wait(m, 2, 1)
        for o in offs:
            if o:
                self.relay(w, self.at_z(o), self.y, missing, col, m, 3, self.sib)
            for v in self.ypeers:
                self.relay(w, self.at_z(o), v, missing, col, m, 3, self.sib)

    def tick(self, todo):
        for stage, m in todo:
            (self.relay_z, self.relay_y, self.relay_x)[stage](m)

    def arrived(self, t):
        self.wait(t, 3, 1)

    def sent(self, t):
        for stage in range(4):
            self.wait(t, stage, 0)


QKV, ADN, AUP, OUT, UP, DOWN = range(6)
AHEAD = 6
UNIT = (4.1, 3.9, 4.0)


class Plan:
    def __init__(self, groups, pairs, zs, n_rb, n, ahead):
        self.pairs = pairs
        self.proj, self.att = [], []
        cost = [5.0, 3.0]
        need = {1: [0, 1]}
        for g in range(groups):
            for k in range(3):
                self.proj.append(len(cost))
                need[len(cost)] = [2 + 3 * g + k]
                cost.append(3.3)
            self.att.append(len(cost))
            cost += [3.45] * pairs
        done = 2 + 3 * groups
        self.out = len(cost)
        need[self.out] = list(range(done, done + groups))
        cost.append(6.0)
        done += groups
        self.ff = len(cost)
        per = (n - done) // zs
        for f in range(zs):
            need[len(cost)] = list(range(done + f * per, done + (f + 1) * per))
            cost += [3.6] * n_rb
        self.end = len(cost)
        cost += [3.6] * n_rb
        self.steps = len(cost)
        self.ticks = {}
        self.spread(cost, need, n, ahead)

    def spread(self, cost, need, n, ahead):
        hop, now = 1.5, 2.0
        free = [now, now, now]
        due = [{}, {}, {}]
        nxt = [0, 0, 0]
        ready = {}

        def begin(c, t):
            free[0] = max(free[0], t) + UNIT[0]
            due[0][c] = free[0] + hop
            free[1] = max(free[1], t) + UNIT[1] / 4

        def run(stage, t):
            c = nxt[stage]
            nxt[stage] += 1
            if stage == 0:
                if c + ahead < n:
                    begin(c + ahead, t)
                free[1] = max(free[1], t) + UNIT[1] * 0.75
                due[1][c] = free[1] + hop
                free[2] = max(free[2], t) + UNIT[2] * 0.43
            elif stage == 1:
                free[2] = max(free[2], t) + UNIT[2] * 0.57
                due[2][c] = free[2] + hop
            else:
                ready[c] = t + 2.0
            return (stage, c)

        def open_ops():
            return [(due[k][nxt[k]], k) for k in range(3) if nxt[k] in due[k]]

        for c in range(min(n, ahead)):
            begin(c, now)
        for step, spent in enumerate(cost):
            todo = []
            if step:
                wanted = need.get(step, [])
                if step == len(cost) - 1:
                    wanted = range(n)
                while True:
                    ops = [v for v in open_ops() if v[0] <= now]
                    if not ops:
                        if all(c in ready for c in wanted):
                            break
                        ops = open_ops()
                    at, stage = min(ops)
                    now = max(now, at)
                    todo.append(run(stage, now))
                for c in wanted:
                    now = max(now, ready[c])
            if todo:
                self.ticks[step] = todo
            now += spent
        self.estimate = now


def layer_body(
    zs, ys, tile, chunks, plan, n_rb, len_ref, id_ref, x_ref, cot_ref, g1_ref, g_ref, qkv_s, adn_s, aup_s, out_s, up_s, down_s,
    qkv_f, proj_ref, inner_ref, adn_ref, aup_ref, ctx_ref, p_ref, y_ref, gh_ref, gc_ref, dgrad_ref, ugrad_ref,
    qa, qb, out_v, up_v, down_v, hid, mlp_acc, gn_acc, nt, io, local, qsem, *sems,
):
    step = pl.program_id(0)
    seq, dim = x_ref.shape
    rows = seq // n_rb
    span = up_v.shape[3] // zs
    mover = Mover(zs, ys, (qkv_s, adn_s, aup_s, out_s, up_s, down_s), (qkv_f, qa, qb, out_v, up_v, down_v), sems, chunks, AHEAD)
    own = [
        pltpu.make_async_copy(src, land.at[mover.z, mover.y], local.at[i])
        for i, (src, land) in enumerate(zip(mover.shards, mover.lands))
    ]

    @pl.when(step == 0)
    def _():
        for cp in own:
            cp.start()
        mover.barrier()
        mover.begin()

        def one(i, carry):
            sl = pl.ds(pl.multiple_of(i * rows, rows), rows)
            unit, _ = norm_stats(x_ref[sl, :].astype(F32))
            nt[sl, :] = (unit * g1_ref[...]).astype(BF)
            return carry

        lax.fori_loop(0, n_rb, one, 0)
        for cp in own:
            cp.wait()

    for at, todo in plan.ticks.items():

        @pl.when(step == at)
        def _():
            mover.tick(todo)

    @pl.when(step == 1)
    def _():
        for t in range(2):
            mover.arrived(t)
        wide = qa.shape[3]
        pick = lax.broadcasted_iota(jnp.int32, (wide, COLS), 0) == lax.broadcasted_iota(jnp.int32, (wide, COLS), 1) + id_ref[0] * COLS
        pick = jnp.where(pick, 1.0, 0.0).astype(BF)
        adn_ref[...] = dense(qa[...].reshape(dim, wide), pick).astype(BF)
        aup_ref[...] = dense(qb[...].reshape(dim, wide), pick).astype(BF)
        inner_ref[...] = dense(nt[...], adn_ref[...]).astype(BF)
        for t in range(2):
            mover.sent(t)

    part = qa.shape[3]
    for i, at in enumerate(plan.proj):
        c0 = (i % 3) * dim + (i // 3) * part
        buf = (qa, qb)[i % 2]

        @pl.when(step == at)
        def _():
            mover.arrived(2 + i)
            cp = pltpu.make_async_copy(qkv_f.at[:, :, :, pl.ds(c0, part)], buf, qsem)
            cp.start()
            cp.wait()

            def one(b, carry):
                sl = pl.ds(pl.multiple_of(b * rows, rows), rows)
                w = buf[...].reshape(dim, part)
                inner = lane_group(inner_ref[sl, :], RANK, i % 3)
                proj_ref[sl, pl.ds(c0, part)] = (
                    dense(nt[sl, :], w) + dense_trans(inner, aup_ref[pl.ds((i // 3) * part, part), :])
                ).astype(BF)
                return carry

            lax.fori_loop(0, n_rb, one, 0)

    lanes = dim // (plan.pairs * len(plan.att))
    for g, base in enumerate(plan.att):

        @pl.when((step >= base) & (step < base + plan.pairs))
        def _():
            first = (step - base + g * plan.pairs) * lanes

            def cut(ref, third):
                return ref.at[:, pl.ds(pl.multiple_of(third * dim + first, 128), lanes)]

            attn_fwd_body(tile, cut(proj_ref, 0), cut(proj_ref, 1), cut(proj_ref, 2), cut(ctx_ref, 0), p_ref)

    def valid_rows(first):
        return first + lax.broadcasted_iota(jnp.int32, (rows, 1), 0) < len_ref[0]

    @pl.when(step == plan.out)
    def _():
        for t in range(len(chunks)):
            if chunks[t][0] == OUT:
                mover.arrived(t)

        def one(i, carry):
            sl = pl.ds(pl.multiple_of(i * rows, rows), rows)
            ctx = ctx_ref[sl, :]
            inner_out = lane_group(dense(ctx, adn_ref[...]), RANK, 3).astype(BF)
            io[sl, :] = inner_out
            hidden = x_ref[sl, :].astype(F32) + (dense(ctx, out_v[...].reshape(dim, dim)) + dense_trans(inner_out, aup_ref[...]))
            hid[sl, :] = hidden
            unit, _ = norm_stats(hidden)
            nt[sl, :] = (unit * g_ref[...]).astype(BF)
            return carry

        lax.fori_loop(0, n_rb, one, 0)

    for k in range(zs):

        @pl.when(step == plan.ff + k * n_rb)
        def _():
            for t in range(len(chunks)):
                if chunks[t][0] == DOWN and chunks[t][1] == (k,) or chunks[t][0] == UP and chunks[t][5][0] == k:
                    mover.arrived(t)

    @pl.when((step >= plan.ff) & (step < plan.end))
    def _():
        at = step - plan.ff
        fz = lax.rem(mover.z + at // n_rb, zs)
        first = lax.rem(at, n_rb) * rows
        sl = pl.ds(pl.multiple_of(first, rows), rows)
        cot = cot_ref[...]
        grad_mlp = jnp.where(valid_rows(first), cot, jnp.zeros_like(cot))
        sub = min(512, span)
        shard_rows = down_v.shape[2]
        k0 = 0.7978845608028654
        for h in range(span // sub):
            up_w = up_v[:, :, :, pl.ds(pl.multiple_of(fz * span + h * sub, 128), sub)].reshape(dim, sub)
            per = sub // shard_rows
            if per:
                down_w = down_v[fz, pl.ds(h * per, per)].reshape(sub, dim)
            else:
                down_w = down_v[fz, h * sub // shard_rows, pl.ds(h * sub % shard_rows, sub)]
            u = dense(nt[sl, :], up_w)
            ga = dense_trans(grad_mlp, down_w)
            sq = u * u
            t = jnp.tanh(k0 * (u + 0.044715 * u * sq))
            half = 0.5 * (1.0 + t)
            act = (u * half).astype(BF)
            d = half + 0.5 * u * (1.0 - t * t) * (k0 * (1.0 + (3.0 * 0.044715) * sq))
            gp = (ga * d).astype(BF)
            m_new = dense(act, down_w)
            g_new = dense_trans(gp, up_w)
            if h == 0:

                @pl.when(at < n_rb)
                def _():
                    mlp_acc[sl, :] = m_new
                    gn_acc[sl, :] = g_new

                @pl.when(at >= n_rb)
                def _():
                    mlp_acc[sl, :] += m_new
                    gn_acc[sl, :] += g_new
            else:
                mlp_acc[sl, :] += m_new
                gn_acc[sl, :] += g_new

    @pl.when(step >= plan.end)
    def _():
        first = (step - plan.end) * rows
        sl = pl.ds(pl.multiple_of(first, rows), rows)
        valid = valid_rows(first)
        hidden = hid[sl, :]
        cot = cot_ref[...]
        y_ref[...] = jnp.where(valid, hidden + mlp_acc[sl, :], 0.0).astype(BF)
        unit, rs = norm_stats(hidden)
        gh = jnp.where(valid, cot, jnp.zeros_like(cot)).astype(F32) + norm_back(unit, rs, g_ref[...], gn_acc[sl, :])
        gh_ref[...] = gh
        ga = gh.astype(BF)
        gio = lane_group(dense(ga, aup_ref[...]), RANK, 3).astype(BF)
        gc_ref[...] = (dense_trans(ga, out_v[...].reshape(dim, dim)) + dense_trans(gio, adn_ref[...])).astype(BF)

        @pl.when(step == plan.end)
        def _():
            dgrad_ref[...] = jnp.zeros_like(dgrad_ref)
            ugrad_ref[...] = jnp.zeros_like(ugrad_ref)

        dgrad_ref[...] += dense_left(gio, ctx_ref[sl, :])
        ugrad_ref[...] += dense_left(io[sl, :], ga)

    @pl.when(step == pl.num_programs(0) - 1)
    def _():
        for t in range(2, len(chunks)):
            mover.sent(t)


def layer(length, adapter, x, cot, gain_one, gain_two, shard_set, n_rep, n_shard, tile, lanes=128, n_rb=4):
    zs, ys = mesh_split(n_rep, n_shard)
    qkv_s, adn_s, aup_s, out_s, up_s, down_s = shard_set
    seq, dim = x.shape
    ff = up_s.shape[1]
    heads = lanes // HEAD
    packed = tile * (seq // tile) * (seq // tile + 1) // 2
    rows = seq // n_rb
    span = ff // zs
    every = tuple(range(zs))
    part = adn_s.shape[1]
    chunks = [(w, every, adn_s.shape[0], 0, part, None) for w in (ADN, AUP)]
    for c in range(0, dim, part):
        chunks += [(QKV, every, qkv_s.shape[0], k * dim + c, part, None) for k in range(3)]
    chunks += [(OUT, every, out_s.shape[0], c, part, None) for c in range(0, dim, part)]
    for k in range(zs):
        chunks += [(DOWN, (k,), down_s.shape[0], c, part, None) for c in range(0, dim, part)]
        chunks += [(UP, every, up_s.shape[0], c, part, (k, span)) for c in range(0, span, part)]
    n = len(chunks)
    plan = Plan(dim // part, part // lanes, zs, n_rb, n, AHEAD)

    def whole(shape):
        return pl.BlockSpec(shape, lambda j: (0, 0), pipeline_mode=pl.Buffered(1))

    def late(j):
        return (jnp.maximum(j - plan.end, 0), 0)

    def pair(j):
        at = jnp.minimum(jnp.maximum(j - plan.att[0], 0), plan.pairs - 1)
        for base in plan.att[1:]:
            at = at + jnp.minimum(jnp.maximum(j - base + 1, 0), plan.pairs)
        return (at, 0, 0)

    row = pl.BlockSpec((rows, dim), late)
    hbm = pl.BlockSpec(memory_space=pl.ANY)
    smem = pl.BlockSpec(memory_space=pltpu.SMEM)
    return pl.pallas_call(
        functools.partial(layer_body, zs, ys, tile, chunks, plan, n_rb),
        grid=(plan.steps,),
        out_shape=[
            jax.ShapeDtypeStruct((zs, ys) + qkv_s.shape, BF),
            jax.ShapeDtypeStruct((seq, 3 * dim), BF),
            jax.ShapeDtypeStruct((seq, COLS), BF),
            jax.ShapeDtypeStruct((dim, COLS), BF),
            jax.ShapeDtypeStruct((dim, COLS), BF),
            jax.ShapeDtypeStruct((seq, dim), BF),
            jax.ShapeDtypeStruct((dim // HEAD, tile, packed), BF),
            jax.ShapeDtypeStruct((seq, dim), BF),
            jax.ShapeDtypeStruct((seq, dim), F32),
            jax.ShapeDtypeStruct((seq, dim), BF),
            jax.ShapeDtypeStruct((COLS, dim), F32),
            jax.ShapeDtypeStruct((COLS, dim), F32),
        ],
        in_specs=[
            smem, smem, whole((seq, dim)),
            pl.BlockSpec((rows, dim), lambda j: (lax.rem(jnp.maximum(j - plan.ff, 0), n_rb), 0)),
            whole((1, dim)), whole((1, dim)), pl.BlockSpec(memory_space=pltpu.VMEM),
            hbm, hbm, hbm, hbm, hbm,
        ],
        out_specs=[
            hbm, whole((seq, 3 * dim)), whole((seq, COLS)), whole((dim, COLS)), whole((dim, COLS)), whole((seq, dim)),
            pl.BlockSpec((heads, tile, packed), pair),
            row, row, row, whole((COLS, dim)), whole((COLS, dim)),
        ],
        scratch_shapes=[
            pltpu.VMEM((zs, ys) + adn_s.shape, BF),
            pltpu.VMEM((zs, ys) + aup_s.shape, BF),
            pltpu.VMEM((zs, ys) + out_s.shape, BF),
            pltpu.VMEM((zs, ys) + up_s.shape, BF),
            pltpu.VMEM((zs, ys) + down_s.shape, BF),
            pltpu.VMEM((seq, dim), F32),
            pltpu.VMEM((seq, dim), F32),
            pltpu.VMEM((seq, dim), F32),
            pltpu.VMEM((seq, dim), BF),
            pltpu.VMEM((seq, COLS), BF),
            pltpu.SemaphoreType.DMA((6,)),
            pltpu.SemaphoreType.DMA,
        ]
        + [pltpu.SemaphoreType.DMA((n,))] * 8,
        compiler_params=pltpu.CompilerParams(collective_id=0, has_side_effects=True, vmem_limit_bytes=66_500_000),
        name="layer_with_gather",
    )(length, adapter, x, cot, gain_one, gain_two, qkv_s, adn_s, aup_s, out_s, up_s, down_s)


def one_slot(tokens, slot_cot, length, adapter, shard_set, gain_one, gain_two, n_rep, n_shard):
    tile = 256 if tokens.shape[0] % 256 == 0 else tokens.shape[0]
    g_one, g_two = gain_one[None], gain_two[None]
    qkv, proj, inner, adn, aup, ctx, probs, y, gh, gc, dg, ug = layer(
        length, adapter, tokens, slot_cot, g_one, g_two, shard_set, n_rep, n_shard, tile
    )
    dq, dk, dv = attention_backward(proj, gc, ctx, probs, tile)
    qkv = qkv.reshape(-1, qkv.shape[-1])
    gx, pay = tail_backward(tokens, gh, inner, dq, dk, dv, g_one, qkv, adn, aup, dg, ug, adapter, n_shard)
    return y, gx, pay


PAY = 2 * COLS + 16


def flip(value, bit):
    return value + bit - 2 * bit * lax.rem(value // bit, 2)


def reduce_body(n_rep, n_shard, bits, pay_ref, down_ref, up_ref, buf, send, recv, xsend, xrecv, lsem):
    r = lax.axis_index("rep")
    s = lax.axis_index("shard")
    others = [lax.rem(s + k, n_shard) for k in range(1, n_shard)]
    peers = [(r, o) for o in others] + [(flip(r, b), s) for b in bits]
    own = pltpu.make_async_copy(pay_ref.at[s], buf.at[r, s], lsem)
    own.start()
    bar = pltpu.get_barrier_semaphore()
    for p in peers:
        pl.semaphore_signal(bar, inc=1, device_id=p, device_id_type=MESH)
    pl.semaphore_wait(bar, len(peers))
    copies = []
    for k, o in enumerate(others):
        cp = pltpu.make_async_remote_copy(
            src_ref=pay_ref.at[o], dst_ref=buf.at[r, s], send_sem=send.at[k], recv_sem=recv.at[k],
            device_id=(r, o), device_id_type=MESH,
        )
        cp.start()
        copies.append(cp)
    own.wait()
    for cp in copies:
        cp.wait()
    held = [0]
    at = 0
    for b in bits:
        partner = flip(r, b)
        copies = []
        for m in held:
            q = r
            for c in bits:
                if m & c:
                    q = flip(q, c)
            cp = pltpu.make_async_remote_copy(
                src_ref=buf.at[q], dst_ref=buf.at[q], send_sem=xsend.at[at], recv_sem=xrecv.at[at],
                device_id=(partner, s), device_id_type=MESH,
            )
            cp.start()
            copies.append(cp)
            at += 1
        for cp in copies:
            cp.wait()
        held = held + [m | b for m in held]
    rows = buf.shape[3]
    for a in range(ADAPTERS):

        def add(i, acc):
            low = buf[i // n_shard, lax.rem(i, n_shard)]
            block = low[: 2 * COLS, :].astype(F32)
            mark = low[2 * COLS : 2 * COLS + 8, :].astype(F32)[0:1, :]
            return acc + jnp.where(mark == float(a), block, 0.0)

        total = lax.fori_loop(0, n_rep * n_shard, add, jnp.zeros((2 * COLS, rows), F32), unroll=4)
        flat = jnp.transpose(total)
        down_ref[:, pl.ds(a * COLS, COLS)] = flat[:, :COLS]
        up_ref[:, pl.ds(a * COLS, COLS)] = flat[:, COLS:]


def reduce_grads(pay, n_rep, n_shard):
    bits = [1 << k for k in range(1, n_rep.bit_length() - 1)] + [1]
    rows = pay.shape[2]
    return pl.pallas_call(
        functools.partial(reduce_body, n_rep, n_shard, bits),
        out_shape=[jax.ShapeDtypeStruct((rows, ADAPTERS * COLS), F32)] * 2,
        in_specs=[pl.BlockSpec(memory_space=pltpu.VMEM)],
        out_specs=[pl.BlockSpec(memory_space=pltpu.VMEM)] * 2,
        scratch_shapes=[pltpu.VMEM((n_rep, n_shard, PAY, rows), BF)]
        + [pltpu.SemaphoreType.DMA((n_shard - 1,))] * 2
        + [pltpu.SemaphoreType.DMA((n_rep - 1,))] * 2
        + [pltpu.SemaphoreType.DMA],
        compiler_params=pltpu.CompilerParams(collective_id=1, has_side_effects=True, vmem_limit_bytes=VMEM_CAP),
        name="reduce_grads",
    )(pay)


def shards(
    inputs,
    cotangent,
    lengths,
    adapter_ids,
    gain_one,
    gain_two,
    qkv_weight,
    out_weight,
    up_weight,
    down_weight,
    adapter_down,
    adapter_up,
):
    n_rep, n_shard = lax.axis_size("rep"), lax.axis_size("shard")
    shard_set = (qkv_weight, adapter_down, adapter_up, out_weight, up_weight, down_weight)
    output, grad, pay = one_slot(
        inputs[0], cotangent[0], lengths, adapter_ids, shard_set, gain_one, gain_two, n_rep, n_shard
    )
    down_grad, up_grad = reduce_grads(pay, n_rep, n_shard)
    return (output[None], grad[None], down_grad, up_grad)


def solution(mesh):
    return jax.shard_map(
        shards,
        mesh=mesh,
        in_specs=(
            P(("rep", "shard"), None, None),
            P(("rep", "shard"), None, None),
            P(("rep", "shard")),
            P(("rep", "shard")),
            P(),
            P(),
            P("shard", None),
            P("shard", None),
            P("shard", None),
            P("shard", None),
            P("shard", None),
            P("shard", None),
        ),
        out_specs=(
            P(("rep", "shard"), None, None),
            P(("rep", "shard"), None, None),
            P("shard", None),
            P("shard", None),
        ),
        check_vma=False,
    )
```

```python
import functools

import jax
import jax.numpy as jnp
from jax import lax
from jax.experimental import pallas as pl
from jax.experimental.pallas import tpu as pltpu
from jax.sharding import PartitionSpec as P

MESH = pl.DeviceIdType.MESH

def mesh_split(n_rep, n_shard):
    zs = 4 if n_shard % 4 == 0 else n_shard
    return zs, n_shard // zs

def share_rows(rows):
    return max(16, rows * 3 // 8 // 16 * 16)


EPS = 1e-05
HEAD = 64
RANK = 16
ADAPTERS = 8
COLS = 4 * RANK
VMEM_CAP = 60 * 1024 * 1024
BF = jnp.bfloat16
F32 = jnp.float32


def dense(left, right):
    return jnp.dot(left, right, preferred_element_type=F32)


def dense_trans(left, right):
    return lax.dot_general(left, right, (((1,), (1,)), ((), ())), preferred_element_type=F32)


def dense_left(left, right):
    return lax.dot_general(left, right, (((0,), (0,)), ((), ())), preferred_element_type=F32)


def lane_group(values, size, group):
    lanes = lax.broadcasted_iota(jnp.int32, values.shape, 1)
    return jnp.where(lanes // size == group, values, jnp.zeros_like(values))


def norm_stats(values):
    center = values - jnp.mean(values, axis=-1, keepdims=True)
    rs = lax.rsqrt(jnp.mean(center * center, axis=-1, keepdims=True) + EPS)
    return center * rs, rs


def norm_back(unit, rs, gain, grad):
    eg = grad * gain
    return rs * (eg - jnp.mean(eg, axis=-1, keepdims=True) - unit * jnp.mean(eg * unit, axis=-1, keepdims=True))


def attn_fwd_body(tile, q_ref, k_ref, v_ref, ctx_ref, p_ref):
    seq, lanes = q_ref.shape
    heads = lanes // HEAD
    scale = HEAD ** (-0.5)
    rows = lax.broadcasted_iota(jnp.int32, (tile, tile), 0)
    cols = lax.broadcasted_iota(jnp.int32, (tile, tile), 1)
    keep = rows >= cols
    off = 0
    for i in range(seq // tile):
        stop = (i + 1) * tile
        q = q_ref[pl.ds(i * tile, tile), :] * jnp.asarray(scale, BF)
        acc = None
        for h in range(heads):
            qh = lane_group(q, HEAD, h)
            s = dense_trans(qh, k_ref[pl.ds(0, stop), :])
            diag = jnp.where(keep, s[:, stop - tile :], -1e30)
            s = diag if i == 0 else jnp.concatenate([s[:, : stop - tile], diag], axis=1)
            peak = jnp.max(s, axis=-1, keepdims=True)
            e = jnp.exp(s - peak)
            inv = 1.0 / jnp.sum(e, axis=-1, keepdims=True)
            p = (e * inv).astype(BF)
            p_ref[h, :, pl.ds(off, stop)] = p
            o = dense(p, lane_group(v_ref[pl.ds(0, stop), :], HEAD, h))
            acc = o if acc is None else acc + o
        ctx_ref[pl.ds(i * tile, tile), :] = acc.astype(BF)
        off += stop


def attn_bwd_body(
    tile, q_ref, k_ref, v_ref, go_ref, ctx_ref, p_ref, y_ref, dq_ref, dk_ref, dv_ref, keep_ref, dk_acc, dv_acc
):
    keep_ref[...] = y_ref[...]
    seq, lanes = q_ref.shape
    heads = lanes // HEAD
    scale = HEAD ** (-0.5)
    off = 0
    n = seq // tile
    dk_acc[...] = jnp.zeros_like(dk_acc)
    dv_acc[...] = jnp.zeros_like(dv_acc)
    for i in range(n):
        stop = (i + 1) * tile
        sl = pl.ds(i * tile, tile)
        past = pl.ds(0, stop)
        go = go_ref[sl, :]
        q = q_ref[sl, :]
        prod = go.astype(F32) * ctx_ref[sl, :].astype(F32)
        acc = None
        for h in range(heads):
            delta = jnp.sum(lane_group(prod, HEAD, h), axis=-1, keepdims=True)
            gh = lane_group(go, HEAD, h)
            p = p_ref[h, :, pl.ds(off, stop)]
            dp = dense_trans(gh, v_ref[past, :])
            ds = (p.astype(F32) * (dp - delta)).astype(BF)
            dv_acc[past, :] += dense_left(p, gh)
            dk_acc[past, :] += dense_left(ds, lane_group(q, HEAD, h))
            o = dense(ds, lane_group(k_ref[past, :], HEAD, h))
            acc = o if acc is None else acc + o
        dq_ref[sl, :] = (acc * scale).astype(BF)
        off += stop
    dk_ref[...] = (dk_acc[...] * scale).astype(BF)
    dv_ref[...] = dv_acc[...].astype(BF)


def attention_backward(proj, grad_ctx, ctx, probs, y, tile, lanes=128):
    seq = proj.shape[0]
    width = proj.shape[1] // 3
    n = width // lanes
    heads = lanes // HEAD
    packed = probs.shape[2]
    blk = pl.BlockSpec((seq, lanes), lambda j: (0, j))
    part = pl.BlockSpec((seq // n, width), lambda j: (j, 0))
    return pl.pallas_call(
        functools.partial(attn_bwd_body, tile),
        grid=(n,),
        out_shape=[jax.ShapeDtypeStruct((seq, width), BF)] * 4,
        in_specs=[pl.BlockSpec((seq, lanes), lambda j, t=t: (0, t * n + j)) for t in range(3)]
        + [blk, blk, pl.BlockSpec((heads, tile, packed), lambda j: (j, 0, 0)), part],
        out_specs=[blk, blk, blk, part],
        scratch_shapes=[pltpu.VMEM((seq, lanes), F32)] * 2,
        compiler_params=pltpu.CompilerParams(vmem_limit_bytes=VMEM_CAP),
        name="attention_backward",
    )(proj, proj, proj, grad_ctx, ctx, probs, y)


class Mover:
    def __init__(self, zs, ys, shards, lands, sems, chunks, ahead):
        self.ahead = ahead
        self.zs, self.ys, self.shards, self.lands, self.sems, self.chunks = zs, ys, shards, lands, sems, chunks
        self.r = lax.axis_index("rep")
        self.s = lax.axis_index("shard")
        self.z, self.y = self.s // ys, lax.rem(self.s, ys)
        self.core = lax.rem(self.r, 2)
        self.xp = lax.rem(self.r // 2, 2)
        self.sib = (self.r + 1 - 2 * self.core, self.s)
        self.par = (self.r + 2 - 4 * self.xp, self.s)
        self.ypeers = [lax.rem(self.y + k, ys) for k in range(1, ys)]

    def at_z(self, off):
        return lax.rem(self.z + off, self.zs)

    def barrier(self):
        peers = [(self.r, self.at_z(k) * self.ys + self.y) for k in range(1, self.zs)]
        peers += [(self.r, self.z * self.ys + v) for v in self.ypeers] + [self.par, self.sib]
        bar = pltpu.get_barrier_semaphore()
        for p in peers:
            pl.semaphore_signal(bar, inc=1, device_id=p, device_id_type=MESH)
        pl.semaphore_wait(bar, len(peers))

    def geom(self, t, dest_z):
        w, offs, rows, c0, cols, turn = self.chunks[t]
        a = share_rows(rows)
        half = cols // 2
        mine = pl.ds(pl.multiple_of(self.xp * a, 16), rows - a)
        excl = pl.ds(pl.multiple_of(self.xp * (rows - a), 16), a)
        missing = pl.ds(pl.multiple_of((1 - self.xp) * (rows - a), 16), a)
        first = c0 + self.core * half
        if turn is not None:
            k, span = turn
            first = first + lax.rem(dest_z + k, self.zs) * span
        return w, offs, rows, a, half, mine, excl, missing, pl.ds(pl.multiple_of(first, 128), half)

    def send(self, src, w, zz, yy, rows, col, t, stage, device):
        pltpu.make_async_remote_copy(
            src_ref=src, dst_ref=self.lands[w].at[zz, yy, rows, col], send_sem=self.sems[2 * stage].at[t],
            recv_sem=self.sems[2 * stage + 1].at[t], device_id=device, device_id_type=MESH,
        ).start()

    def relay(self, w, zz, yy, rows, col, t, stage, device):
        self.send(self.lands[w].at[zz, yy, rows, col], w, zz, yy, rows, col, t, stage, device)

    def wait(self, t, stage, side):
        w, offs, rows, a, half, *_ = self.geom(t, self.z)
        far = len([o for o in offs if o])
        near = len(offs) * (self.ys - 1)
        count = ((far * (rows - a)), near * (rows - a), (far + near) * a, (far + near) * rows)[stage]
        if count == 0:
            return
        sem = self.sems[2 * stage + side].at[t]
        elems = count * half
        for out in self.lands:
            _, _, big_r, big_n = out.shape
            for lead in range(1, self.zs + 1):
                for take in range(big_r, 0, -16):
                    if elems % (lead * take * 128) == 0 and elems // (lead * take) <= big_n:
                        reg = out.at[pl.ds(0, lead), 0, pl.ds(0, take), pl.ds(0, elems // (lead * take))]
                        pltpu.make_async_copy(reg, reg, sem).wait()
                        return
        raise ValueError("no region")

    def start_z(self, t):
        offs = self.chunks[t][1]
        for k in range(1, self.zs):
            if (self.zs - k) % self.zs in offs:
                zz = self.at_z(k)
                w, _, _, _, _, mine, _, _, col = self.geom(t, zz)
                self.send(self.shards[w].at[mine, col], w, self.z, self.y, mine, col, t, 0, (self.r, zz * self.ys + self.y))

    def start_y(self, t):
        w, offs, _, _, _, mine, _, _, col = self.geom(t, self.z)
        if 0 in offs:
            for v in self.ypeers:
                self.send(self.shards[w].at[mine, col], w, self.z, self.y, mine, col, t, 1, (self.r, self.z * self.ys + v))

    def begin(self):
        for t in range(min(self.ahead, len(self.chunks))):
            self.start_z(t)
            self.start_y(t)

    def relay_z(self, m):
        if m + self.ahead < len(self.chunks):
            self.start_z(m + self.ahead)
            self.start_y(m + self.ahead)
        w, offs, rows, a, half, mine, excl, missing, col = self.geom(m, self.z)
        self.wait(m, 0, 1)
        for o in offs:
            if o:
                for v in self.ypeers:
                    self.relay(w, self.at_z(o), self.y, mine, col, m, 1, (self.r, self.z * self.ys + v))
        for o in offs:
            if o:
                self.relay(w, self.at_z(o), self.y, excl, col, m, 2, self.par)
                self.relay(w, self.at_z(o), self.y, mine, col, m, 3, self.sib)

    def relay_y(self, m):
        w, offs, rows, a, half, mine, excl, missing, col = self.geom(m, self.z)
        self.wait(m, 1, 1)
        for o in offs:
            for v in self.ypeers:
                self.relay(w, self.at_z(o), v, excl, col, m, 2, self.par)
                self.relay(w, self.at_z(o), v, mine, col, m, 3, self.sib)

    def relay_x(self, m):
        w, offs, rows, a, half, mine, excl, missing, col = self.geom(m, self.z)
        self.wait(m, 2, 1)
        for o in offs:
            if o:
                self.relay(w, self.at_z(o), self.y, missing, col, m, 3, self.sib)
            for v in self.ypeers:
                self.relay(w, self.at_z(o), v, missing, col, m, 3, self.sib)

    def tick(self, todo):
        for stage, m in todo:
            (self.relay_z, self.relay_y, self.relay_x)[stage](m)

    def arrived(self, t):
        self.wait(t, 3, 1)

    def sent(self, t):
        for stage in range(4):
            self.wait(t, stage, 0)


QKV, ADN, AUP, OUT, UP, DOWN = range(6)
AHEAD = 6
UNIT = (4.1, 3.9, 4.0)


class Plan:
    def __init__(self, groups, pairs, zs, n_rb, n, ahead):
        self.pairs = pairs
        self.proj, self.att = [], []
        cost = [5.0, 3.0]
        need = {1: [0, 1]}
        for g in range(groups):
            for k in range(3):
                self.proj.append(len(cost))
                need[len(cost)] = [2 + 3 * g + k]
                cost.append(3.3)
            self.att.append(len(cost))
            cost += [3.45] * pairs
        done = 2 + 3 * groups
        self.out = len(cost)
        need[self.out] = list(range(done, done + groups))
        cost.append(6.0)
        done += groups
        self.ff = len(cost)
        per = (n - done) // zs
        for f in range(zs):
            need[len(cost)] = list(range(done + f * per, done + (f + 1) * per))
            cost += [3.6] * n_rb
        self.end = len(cost)
        cost += [3.6] * n_rb
        self.steps = len(cost)
        self.ticks = {}
        self.spread(cost, need, n, ahead)

    def spread(self, cost, need, n, ahead):
        hop, now = 1.5, 2.0
        free = [now, now, now]
        due = [{}, {}, {}]
        nxt = [0, 0, 0]
        ready = {}

        def begin(c, t):
            free[0] = max(free[0], t) + UNIT[0]
            due[0][c] = free[0] + hop
            free[1] = max(free[1], t) + UNIT[1] / 4

        def run(stage, t):
            c = nxt[stage]
            nxt[stage] += 1
            if stage == 0:
                if c + ahead < n:
                    begin(c + ahead, t)
                free[1] = max(free[1], t) + UNIT[1] * 0.75
                due[1][c] = free[1] + hop
                free[2] = max(free[2], t) + UNIT[2] * 0.43
            elif stage == 1:
                free[2] = max(free[2], t) + UNIT[2] * 0.57
                due[2][c] = free[2] + hop
            else:
                ready[c] = t + 2.0
            return (stage, c)

        def open_ops():
            return [(due[k][nxt[k]], k) for k in range(3) if nxt[k] in due[k]]

        for c in range(min(n, ahead)):
            begin(c, now)
        for step, spent in enumerate(cost):
            todo = []
            if step:
                wanted = need.get(step, [])
                if step == len(cost) - 1:
                    wanted = range(n)
                while True:
                    ops = [v for v in open_ops() if v[0] <= now]
                    if not ops:
                        if all(c in ready for c in wanted):
                            break
                        ops = open_ops()
                    at, stage = min(ops)
                    now = max(now, at)
                    todo.append(run(stage, now))
                for c in wanted:
                    now = max(now, ready[c])
            if todo:
                self.ticks[step] = todo
            now += spent
        self.estimate = now


def layer_body(
    zs, ys, tile, chunks, plan, n_rb, len_ref, id_ref, x_ref, cot_ref, g1_ref, g_ref, qkv_s, adn_s, aup_s, out_s, up_s, down_s,
    qkv_f, proj_ref, inner_ref, adn_ref, aup_ref, ctx_ref, p_ref, y_ref, gh_ref, gc_ref, dgrad_ref, ugrad_ref,
    qa, qb, out_v, up_v, down_v, hid, mlp_acc, gn_acc, nt, io, local, qsem, *sems,
):
    step = pl.program_id(0)
    seq, dim = x_ref.shape
    rows = seq // n_rb
    span = up_v.shape[3] // zs
    mover = Mover(zs, ys, (qkv_s, adn_s, aup_s, out_s, up_s, down_s), (qkv_f, qa, qb, out_v, up_v, down_v), sems, chunks, AHEAD)
    own = [
        pltpu.make_async_copy(src, land.at[mover.z, mover.y], local.at[i])
        for i, (src, land) in enumerate(zip(mover.shards, mover.lands))
    ]

    @pl.when(step == 0)
    def _():
        for cp in own:
            cp.start()
        mover.barrier()
        mover.begin()

        def one(i, carry):
            sl = pl.ds(pl.multiple_of(i * rows, rows), rows)
            unit, _ = norm_stats(x_ref[sl, :].astype(F32))
            nt[sl, :] = (unit * g1_ref[...]).astype(BF)
            return carry

        lax.fori_loop(0, n_rb, one, 0)
        for cp in own:
            cp.wait()

    for at, todo in plan.ticks.items():

        @pl.when(step == at)
        def _():
            mover.tick(todo)

    @pl.when(step == 1)
    def _():
        for t in range(2):
            mover.arrived(t)
        wide = qa.shape[3]
        pick = lax.broadcasted_iota(jnp.int32, (wide, COLS), 0) == lax.broadcasted_iota(jnp.int32, (wide, COLS), 1) + id_ref[0] * COLS
        pick = jnp.where(pick, 1.0, 0.0).astype(BF)
        adn_ref[...] = dense(qa[...].reshape(dim, wide), pick).astype(BF)
        aup_ref[...] = dense(qb[...].reshape(dim, wide), pick).astype(BF)
        inner_ref[...] = dense(nt[...], adn_ref[...]).astype(BF)
        for t in range(2):
            mover.sent(t)

    part = qa.shape[3]
    for i, at in enumerate(plan.proj):
        c0 = (i % 3) * dim + (i // 3) * part
        buf = (qa, qb)[i % 2]

        @pl.when(step == at)
        def _():
            mover.arrived(2 + i)
            cp = pltpu.make_async_copy(qkv_f.at[:, :, :, pl.ds(c0, part)], buf, qsem)
            cp.start()
            cp.wait()

            def one(b, carry):
                sl = pl.ds(pl.multiple_of(b * rows, rows), rows)
                w = buf[...].reshape(dim, part)
                inner = lane_group(inner_ref[sl, :], RANK, i % 3)
                proj_ref[sl, pl.ds(c0, part)] = (
                    dense(nt[sl, :], w) + dense_trans(inner, aup_ref[pl.ds((i // 3) * part, part), :])
                ).astype(BF)
                return carry

            lax.fori_loop(0, n_rb, one, 0)

    lanes = dim // (plan.pairs * len(plan.att))
    for g, base in enumerate(plan.att):

        @pl.when((step >= base) & (step < base + plan.pairs))
        def _():
            first = (step - base + g * plan.pairs) * lanes

            def cut(ref, third):
                return ref.at[:, pl.ds(pl.multiple_of(third * dim + first, 128), lanes)]

            attn_fwd_body(tile, cut(proj_ref, 0), cut(proj_ref, 1), cut(proj_ref, 2), cut(ctx_ref, 0), p_ref)

    def valid_rows(first):
        return first + lax.broadcasted_iota(jnp.int32, (rows, 1), 0) < len_ref[0]

    @pl.when(step == plan.out)
    def _():
        for t in range(len(chunks)):
            if chunks[t][0] == OUT:
                mover.arrived(t)

        def one(i, carry):
            sl = pl.ds(pl.multiple_of(i * rows, rows), rows)
            ctx = ctx_ref[sl, :]
            inner_out = lane_group(dense(ctx, adn_ref[...]), RANK, 3).astype(BF)
            io[sl, :] = inner_out
            hidden = x_ref[sl, :].astype(F32) + (dense(ctx, out_v[...].reshape(dim, dim)) + dense_trans(inner_out, aup_ref[...]))
            hid[sl, :] = hidden
            unit, _ = norm_stats(hidden)
            nt[sl, :] = (unit * g_ref[...]).astype(BF)
            return carry

        lax.fori_loop(0, n_rb, one, 0)

    for k in range(zs):

        @pl.when(step == plan.ff + k * n_rb)
        def _():
            for t in range(len(chunks)):
                if chunks[t][0] == DOWN and chunks[t][1] == (k,) or chunks[t][0] == UP and chunks[t][5][0] == k:
                    mover.arrived(t)

    @pl.when((step >= plan.ff) & (step < plan.end))
    def _():
        at = step - plan.ff
        fz = lax.rem(mover.z + at // n_rb, zs)
        first = lax.rem(at, n_rb) * rows
        sl = pl.ds(pl.multiple_of(first, rows), rows)
        cot = cot_ref[...]
        grad_mlp = jnp.where(valid_rows(first), cot, jnp.zeros_like(cot))
        sub = min(512, span)
        shard_rows = down_v.shape[2]
        k0 = 0.7978845608028654
        for h in range(span // sub):
            up_w = up_v[:, :, :, pl.ds(pl.multiple_of(fz * span + h * sub, 128), sub)].reshape(dim, sub)
            per = sub // shard_rows
            if per:
                down_w = down_v[fz, pl.ds(h * per, per)].reshape(sub, dim)
            else:
                down_w = down_v[fz, h * sub // shard_rows, pl.ds(h * sub % shard_rows, sub)]
            u = dense(nt[sl, :], up_w)
            ga = dense_trans(grad_mlp, down_w)
            sq = u * u
            t = jnp.tanh(k0 * (u + 0.044715 * u * sq))
            half = 0.5 * (1.0 + t)
            act = (u * half).astype(BF)
            d = half + 0.5 * u * (1.0 - t * t) * (k0 * (1.0 + (3.0 * 0.044715) * sq))
            gp = (ga * d).astype(BF)
            m_new = dense(act, down_w)
            g_new = dense_trans(gp, up_w)
            if h == 0:

                @pl.when(at < n_rb)
                def _():
                    mlp_acc[sl, :] = m_new
                    gn_acc[sl, :] = g_new

                @pl.when(at >= n_rb)
                def _():
                    mlp_acc[sl, :] += m_new
                    gn_acc[sl, :] += g_new
            else:
                mlp_acc[sl, :] += m_new
                gn_acc[sl, :] += g_new

    @pl.when(step >= plan.end)
    def _():
        first = (step - plan.end) * rows
        sl = pl.ds(pl.multiple_of(first, rows), rows)
        valid = valid_rows(first)
        hidden = hid[sl, :]
        cot = cot_ref[...]
        y_ref[...] = jnp.where(valid, hidden + mlp_acc[sl, :], 0.0).astype(BF)
        unit, rs = norm_stats(hidden)
        gh = jnp.where(valid, cot, jnp.zeros_like(cot)).astype(F32) + norm_back(unit, rs, g_ref[...], gn_acc[sl, :])
        gh_ref[...] = gh
        ga = gh.astype(BF)
        gio = lane_group(dense(ga, aup_ref[...]), RANK, 3).astype(BF)
        gc_ref[...] = (dense_trans(ga, out_v[...].reshape(dim, dim)) + dense_trans(gio, adn_ref[...])).astype(BF)

        @pl.when(step == plan.end)
        def _():
            dgrad_ref[...] = jnp.zeros_like(dgrad_ref)
            ugrad_ref[...] = jnp.zeros_like(ugrad_ref)

        dgrad_ref[...] += dense_left(gio, ctx_ref[sl, :])
        ugrad_ref[...] += dense_left(io[sl, :], ga)

    @pl.when(step == pl.num_programs(0) - 1)
    def _():
        for t in range(2, len(chunks)):
            mover.sent(t)


def layer(length, adapter, x, cot, gain_one, gain_two, shard_set, n_rep, n_shard, tile, lanes=128, n_rb=4):
    zs, ys = mesh_split(n_rep, n_shard)
    qkv_s, adn_s, aup_s, out_s, up_s, down_s = shard_set
    seq, dim = x.shape
    ff = up_s.shape[1]
    heads = lanes // HEAD
    packed = tile * (seq // tile) * (seq // tile + 1) // 2
    rows = seq // n_rb
    span = ff // zs
    every = tuple(range(zs))
    part = adn_s.shape[1]
    chunks = [(w, every, adn_s.shape[0], 0, part, None) for w in (ADN, AUP)]
    for c in range(0, dim, part):
        chunks += [(QKV, every, qkv_s.shape[0], k * dim + c, part, None) for k in range(3)]
    chunks += [(OUT, every, out_s.shape[0], c, part, None) for c in range(0, dim, part)]
    for k in range(zs):
        chunks += [(DOWN, (k,), down_s.shape[0], c, part, None) for c in range(0, dim, part)]
        chunks += [(UP, every, up_s.shape[0], c, part, (k, span)) for c in range(0, span, part)]
    n = len(chunks)
    plan = Plan(dim // part, part // lanes, zs, n_rb, n, AHEAD)

    def whole(shape):
        return pl.BlockSpec(shape, lambda j: (0, 0), pipeline_mode=pl.Buffered(1))

    def late(j):
        return (jnp.maximum(j - plan.end, 0), 0)

    def pair(j):
        at = jnp.minimum(jnp.maximum(j - plan.att[0], 0), plan.pairs - 1)
        for base in plan.att[1:]:
            at = at + jnp.minimum(jnp.maximum(j - base + 1, 0), plan.pairs)
        return (at, 0, 0)

    row = pl.BlockSpec((rows, dim), late)
    hbm = pl.BlockSpec(memory_space=pl.ANY)
    smem = pl.BlockSpec(memory_space=pltpu.SMEM)
    return pl.pallas_call(
        functools.partial(layer_body, zs, ys, tile, chunks, plan, n_rb),
        grid=(plan.steps,),
        out_shape=[
            jax.ShapeDtypeStruct((zs, ys) + qkv_s.shape, BF),
            jax.ShapeDtypeStruct((seq, 3 * dim), BF),
            jax.ShapeDtypeStruct((seq, COLS), BF),
            jax.ShapeDtypeStruct((dim, COLS), BF),
            jax.ShapeDtypeStruct((dim, COLS), BF),
            jax.ShapeDtypeStruct((seq, dim), BF),
            jax.ShapeDtypeStruct((dim // HEAD, tile, packed), BF),
            jax.ShapeDtypeStruct((seq, dim), BF),
            jax.ShapeDtypeStruct((seq, dim), F32),
            jax.ShapeDtypeStruct((seq, dim), BF),
            jax.ShapeDtypeStruct((COLS, dim), F32),
            jax.ShapeDtypeStruct((COLS, dim), F32),
        ],
        in_specs=[
            smem, smem, whole((seq, dim)),
            pl.BlockSpec((rows, dim), lambda j: (lax.rem(jnp.maximum(j - plan.ff, 0), n_rb), 0)),
            whole((1, dim)), whole((1, dim)), pl.BlockSpec(memory_space=pltpu.VMEM),
            hbm, hbm, hbm, hbm, hbm,
        ],
        out_specs=[
            hbm, whole((seq, 3 * dim)), whole((seq, COLS)), whole((dim, COLS)), whole((dim, COLS)), whole((seq, dim)),
            pl.BlockSpec((heads, tile, packed), pair),
            row, row, row, whole((COLS, dim)), whole((COLS, dim)),
        ],
        scratch_shapes=[
            pltpu.VMEM((zs, ys) + adn_s.shape, BF),
            pltpu.VMEM((zs, ys) + aup_s.shape, BF),
            pltpu.VMEM((zs, ys) + out_s.shape, BF),
            pltpu.VMEM((zs, ys) + up_s.shape, BF),
            pltpu.VMEM((zs, ys) + down_s.shape, BF),
            pltpu.VMEM((seq, dim), F32),
            pltpu.VMEM((seq, dim), F32),
            pltpu.VMEM((seq, dim), F32),
            pltpu.VMEM((seq, dim), BF),
            pltpu.VMEM((seq, COLS), BF),
            pltpu.SemaphoreType.DMA((6,)),
            pltpu.SemaphoreType.DMA,
        ]
        + [pltpu.SemaphoreType.DMA((n,))] * 8,
        compiler_params=pltpu.CompilerParams(collective_id=0, has_side_effects=True, vmem_limit_bytes=66_500_000),
        name="layer_with_gather",
    )(length, adapter, x, cot, gain_one, gain_two, qkv_s, adn_s, aup_s, out_s, up_s, down_s)


def one_slot(tokens, slot_cot, length, adapter, shard_set, gain_one, gain_two, n_rep, n_shard):
    tile = 256 if tokens.shape[0] % 256 == 0 else tokens.shape[0]
    g_one, g_two = gain_one[None], gain_two[None]
    qkv, proj, inner, adn, aup, ctx, probs, y, gh, gc, dg, ug = layer(
        length, adapter, tokens, slot_cot, g_one, g_two, shard_set, n_rep, n_shard, tile
    )
    dq, dk, dv, y = attention_backward(proj, gc, ctx, probs, y, tile)
    qkv = qkv.reshape(-1, qkv.shape[-1])
    return y, *tail_backward(tokens, gh, inner, dq, dk, dv, g_one, qkv, adn, aup, dg, ug, adapter, n_rep, n_shard)


PAY = 2 * COLS + 16


def flip(value, bit):
    return value + bit - 2 * bit * lax.rem(value // bit, 2)


def tail_body(
    n_rep, n_shard, bits, nb, x_ref, gh_ref, inner_ref, dq_ref, dk_ref, dv_ref, g_ref, w_ref, adn_ref, aup_ref,
    din_ref, uin_ref, id_ref, gx_ref, down_ref, up_ref, gi_s, dgrad, ugrad, pay, buf, send, recv, xsend, xrecv, lsem,
):
    step = pl.program_id(0)
    rows, dim = x_ref.shape
    r = lax.axis_index("rep")
    s = lax.axis_index("shard")
    others = [lax.rem(s + k, n_shard) for k in range(1, n_shard)]
    peers = [(r, o) for o in others] + [(flip(r, b), s) for b in bits]
    own = pltpu.make_async_copy(pay.at[s], buf.at[r, s], lsem)
    first = [
        pltpu.make_async_remote_copy(
            src_ref=pay.at[o], dst_ref=buf.at[r, s], send_sem=send.at[k], recv_sem=recv.at[k],
            device_id=(r, o), device_id_type=MESH,
        )
        for k, o in enumerate(others)
    ]
    rounds = []
    held, at = [0], 0
    for b in bits:
        copies = []
        for m in held:
            q = r
            for c in bits:
                if m & c:
                    q = flip(q, c)
            copies.append(
                pltpu.make_async_remote_copy(
                    src_ref=buf.at[q], dst_ref=buf.at[q], send_sem=xsend.at[at], recv_sem=xrecv.at[at],
                    device_id=(flip(r, b), s), device_id_type=MESH,
                )
            )
            at += 1
        rounds.append(copies)
        held = held + [m | b for m in held]

    def block_sl():
        return pl.ds(pl.multiple_of(lax.rem(step, nb) * rows, rows), rows)

    @pl.when(step == 0)
    def _():
        dgrad[...] = din_ref[...]
        ugrad[...] = uin_ref[...]

    @pl.when(step < nb)
    def _():
        thirds = [dq_ref[...], dk_ref[...], dv_ref[...]]
        gi, up = None, None
        for p in range(3):
            one = lane_group(dense(thirds[p], aup_ref[...]), RANK, p)
            gi = one if gi is None else gi + one
            two = dense_left(lane_group(inner_ref[...], RANK, p), thirds[p])
            up = two if up is None else up + two
        gi = gi.astype(BF)
        gi_s[block_sl(), :] = gi
        unit, _ = norm_stats(x_ref[...].astype(F32))
        dgrad[...] += dense_left(gi, (unit * g_ref[...]).astype(BF))
        ugrad[...] += up

    @pl.when(step == nb - 1)
    def _():
        width = pay.shape[2]
        mark = jnp.full((PAY - 2 * COLS, width), id_ref[0], jnp.int32).astype(F32)
        for i in range(n_shard):
            sl = pl.ds(i * width, width)
            pay[i] = jnp.concatenate([dgrad[:, sl], ugrad[:, sl], mark], axis=0).astype(BF)
        bar = pltpu.get_barrier_semaphore()
        for p in peers:
            pl.semaphore_signal(bar, inc=1, device_id=p, device_id_type=MESH)
        pl.semaphore_wait(bar, len(peers))

    @pl.when(step == nb)
    def _():
        own.start()
        for cp in first:
            cp.start()

    @pl.when(step == nb + nb // 2)
    def _():
        own.wait()
        for cp in first:
            cp.wait()
        for cp in rounds[0]:
            cp.start()

    @pl.when((step >= nb) & (step < 2 * nb))
    def _():
        thirds = [dq_ref[...], dk_ref[...], dv_ref[...]]
        gn = dense_trans(gi_s[block_sl(), :], adn_ref[...])
        for p in range(3):
            gn = gn + dense_trans(thirds[p], w_ref[:, pl.ds(p * dim, dim)])
        unit, rs = norm_stats(x_ref[...].astype(F32))
        gx_ref[...] = (gh_ref[...] + norm_back(unit, rs, g_ref[...], gn)).astype(BF)

    @pl.when(step == 2 * nb)
    def _():
        for cp in rounds[0]:
            cp.wait()
        for copies in rounds[1:]:
            for cp in copies:
                cp.start()
            for cp in copies:
                cp.wait()
        width = buf.shape[3]
        for a in range(ADAPTERS):

            def add(i, acc):
                low = buf[i // n_shard, lax.rem(i, n_shard)]
                block = low[: 2 * COLS, :].astype(F32)
                mark = low[2 * COLS : 2 * COLS + 8, :].astype(F32)[0:1, :]
                return acc + jnp.where(mark == float(a), block, 0.0)

            total = lax.fori_loop(0, n_rep * n_shard, add, jnp.zeros((2 * COLS, width), F32), unroll=4)
            flat = jnp.transpose(total)
            down_ref[:, pl.ds(a * COLS, COLS)] = flat[:, :COLS]
            up_ref[:, pl.ds(a * COLS, COLS)] = flat[:, COLS:]


def tail_backward(x, gh, inner, dq, dk, dv, gain, qkv, adn, aup, din, uin, adapter, n_rep, n_shard, rows=256):
    seq, dim = x.shape
    nb = seq // rows
    bits = [1 << k for k in range(1, n_rep.bit_length() - 1)] + [1]
    width = dim // n_shard

    def both(j):
        return (lax.rem(jnp.minimum(j, 2 * nb - 1), nb), 0)

    def second(j):
        return (jnp.minimum(jnp.maximum(j - nb, 0), nb - 1), 0)

    def whole(shape):
        return pl.BlockSpec(shape, lambda j: (0, 0), pipeline_mode=pl.Buffered(1))

    row = pl.BlockSpec((rows, dim), both)
    late = pl.BlockSpec((rows, dim), second)
    return pl.pallas_call(
        functools.partial(tail_body, n_rep, n_shard, bits, nb),
        grid=(2 * nb + 1,),
        out_shape=[jax.ShapeDtypeStruct((seq, dim), BF)]
        + [jax.ShapeDtypeStruct((width, ADAPTERS * COLS), F32)] * 2,
        in_specs=[
            row, late, pl.BlockSpec((rows, COLS), both), row, row, row,
            whole((1, dim)), whole(qkv.shape), whole((dim, COLS)), whole((dim, COLS)), whole((COLS, dim)), whole((COLS, dim)),
            pl.BlockSpec(memory_space=pltpu.SMEM),
        ],
        out_specs=[late, whole((width, ADAPTERS * COLS)), whole((width, ADAPTERS * COLS))],
        scratch_shapes=[
            pltpu.VMEM((seq, COLS), BF),
            pltpu.VMEM((COLS, dim), F32),
            pltpu.VMEM((COLS, dim), F32),
            pltpu.VMEM((n_shard, PAY, width), BF),
            pltpu.VMEM((n_rep, n_shard, PAY, width), BF),
        ]
        + [pltpu.SemaphoreType.DMA((n_shard - 1,))] * 2
        + [pltpu.SemaphoreType.DMA((n_rep - 1,))] * 2
        + [pltpu.SemaphoreType.DMA],
        compiler_params=pltpu.CompilerParams(collective_id=1, has_side_effects=True, vmem_limit_bytes=VMEM_CAP),
        name="tail_and_reduce",
    )(x, gh, inner, dq, dk, dv, gain, qkv, adn, aup, din, uin, adapter)


def shards(
    inputs,
    cotangent,
    lengths,
    adapter_ids,
    gain_one,
    gain_two,
    qkv_weight,
    out_weight,
    up_weight,
    down_weight,
    adapter_down,
    adapter_up,
):
    n_rep, n_shard = lax.axis_size("rep"), lax.axis_size("shard")
    shard_set = (qkv_weight, adapter_down, adapter_up, out_weight, up_weight, down_weight)
    output, grad, down_grad, up_grad = one_slot(
        inputs[0], cotangent[0], lengths, adapter_ids, shard_set, gain_one, gain_two, n_rep, n_shard
    )
    return (output[None], grad[None], down_grad, up_grad)


def solution(mesh):
    return jax.shard_map(
        shards,
        mesh=mesh,
        in_specs=(
            P(("rep", "shard"), None, None),
            P(("rep", "shard"), None, None),
            P(("rep", "shard")),
            P(("rep", "shard")),
            P(),
            P(),
            P("shard", None),
            P("shard", None),
            P("shard", None),
            P("shard", None),
            P("shard", None),
            P("shard", None),
        ),
        out_specs=(
            P(("rep", "shard"), None, None),
            P(("rep", "shard"), None, None),
            P("shard", None),
            P("shard", None),
        ),
        check_vma=False,
    )
```

```python
import functools

import jax
import jax.numpy as jnp
from jax import lax
from jax.experimental import pallas as pl
from jax.experimental.pallas import tpu as pltpu
from jax.sharding import PartitionSpec as P

MESH = pl.DeviceIdType.MESH

def mesh_split(n_rep, n_shard):
    zs = 4 if n_shard % 4 == 0 else n_shard
    return zs, n_shard // zs

def share_rows(rows):
    return max(16, rows * 3 // 8 // 16 * 16)


EPS = 1e-05
HEAD = 64
RANK = 16
ADAPTERS = 8
COLS = 4 * RANK
VMEM_CAP = 60 * 1024 * 1024
BF = jnp.bfloat16
F32 = jnp.float32


def dense(left, right):
    return jnp.dot(left, right, preferred_element_type=F32)


def dense_trans(left, right):
    return lax.dot_general(left, right, (((1,), (1,)), ((), ())), preferred_element_type=F32)


def dense_left(left, right):
    return lax.dot_general(left, right, (((0,), (0,)), ((), ())), preferred_element_type=F32)


def lane_group(values, size, group):
    lanes = lax.broadcasted_iota(jnp.int32, values.shape, 1)
    return jnp.where(lanes // size == group, values, jnp.zeros_like(values))


def norm_stats(values):
    center = values - jnp.mean(values, axis=-1, keepdims=True)
    rs = lax.rsqrt(jnp.mean(center * center, axis=-1, keepdims=True) + EPS)
    return center * rs, rs


def norm_back(unit, rs, gain, grad):
    eg = grad * gain
    return rs * (eg - jnp.mean(eg, axis=-1, keepdims=True) - unit * jnp.mean(eg * unit, axis=-1, keepdims=True))


def attn_fwd_body(tile, q_ref, k_ref, v_ref, ctx_ref, p_ref):
    seq, lanes = q_ref.shape
    heads = lanes // HEAD
    scale = HEAD ** (-0.5)
    rows = lax.broadcasted_iota(jnp.int32, (tile, tile), 0)
    cols = lax.broadcasted_iota(jnp.int32, (tile, tile), 1)
    keep = rows >= cols
    off = 0
    for i in range(seq // tile):
        stop = (i + 1) * tile
        q = q_ref[pl.ds(i * tile, tile), :] * jnp.asarray(scale, BF)
        acc = None
        for h in range(heads):
            qh = lane_group(q, HEAD, h)
            s = dense_trans(qh, k_ref[pl.ds(0, stop), :])
            diag = jnp.where(keep, s[:, stop - tile :], -1e30)
            s = diag if i == 0 else jnp.concatenate([s[:, : stop - tile], diag], axis=1)
            peak = jnp.max(s, axis=-1, keepdims=True)
            e = jnp.exp(s - peak)
            inv = 1.0 / jnp.sum(e, axis=-1, keepdims=True)
            p = (e * inv).astype(BF)
            p_ref[h, :, pl.ds(off, stop)] = p
            o = dense(p, lane_group(v_ref[pl.ds(0, stop), :], HEAD, h))
            acc = o if acc is None else acc + o
        ctx_ref[pl.ds(i * tile, tile), :] = acc.astype(BF)
        off += stop


def attn_bwd_body(
    tile, q_ref, k_ref, v_ref, go_ref, ctx_ref, p_ref, y_ref, dq_ref, dk_ref, dv_ref, keep_ref, dk_acc, dv_acc
):
    keep_ref[...] = y_ref[...]
    seq, lanes = q_ref.shape
    heads = lanes // HEAD
    scale = HEAD ** (-0.5)
    off = 0
    n = seq // tile
    dk_acc[...] = jnp.zeros_like(dk_acc)
    dv_acc[...] = jnp.zeros_like(dv_acc)
    for i in range(n):
        stop = (i + 1) * tile
        sl = pl.ds(i * tile, tile)
        past = pl.ds(0, stop)
        go = go_ref[sl, :]
        q = q_ref[sl, :]
        prod = go.astype(F32) * ctx_ref[sl, :].astype(F32)
        acc = None
        for h in range(heads):
            delta = jnp.sum(lane_group(prod, HEAD, h), axis=-1, keepdims=True)
            gh = lane_group(go, HEAD, h)
            p = p_ref[h, :, pl.ds(off, stop)]
            dp = dense_trans(gh, v_ref[past, :])
            ds = (p.astype(F32) * (dp - delta)).astype(BF)
            dv_acc[past, :] += dense_left(p, gh)
            dk_acc[past, :] += dense_left(ds, lane_group(q, HEAD, h))
            o = dense(ds, lane_group(k_ref[past, :], HEAD, h))
            acc = o if acc is None else acc + o
        dq_ref[sl, :] = (acc * scale).astype(BF)
        off += stop
    dk_ref[...] = (dk_acc[...] * scale).astype(BF)
    dv_ref[...] = dv_acc[...].astype(BF)


def attention_backward(proj, grad_ctx, ctx, probs, y, tile, lanes=128):
    seq = proj.shape[0]
    width = proj.shape[1] // 3
    n = width // lanes
    heads = lanes // HEAD
    packed = probs.shape[2]
    blk = pl.BlockSpec((seq, lanes), lambda j: (0, j))
    part = pl.BlockSpec((seq // n, width), lambda j: (j, 0))
    return pl.pallas_call(
        functools.partial(attn_bwd_body, tile),
        grid=(n,),
        out_shape=[jax.ShapeDtypeStruct((seq, width), BF)] * 4,
        in_specs=[pl.BlockSpec((seq, lanes), lambda j, t=t: (0, t * n + j)) for t in range(3)]
        + [blk, blk, pl.BlockSpec((heads, tile, packed), lambda j: (j, 0, 0)), part],
        out_specs=[blk, blk, blk, part],
        scratch_shapes=[pltpu.VMEM((seq, lanes), F32)] * 2,
        compiler_params=pltpu.CompilerParams(vmem_limit_bytes=VMEM_CAP),
        name="attention_backward",
    )(proj, proj, proj, grad_ctx, ctx, probs, y)


class Mover:
    def __init__(self, zs, ys, shards, lands, sems, chunks, ahead):
        self.ahead = ahead
        self.zs, self.ys, self.shards, self.lands, self.sems, self.chunks = zs, ys, shards, lands, sems, chunks
        self.r = lax.axis_index("rep")
        self.s = lax.axis_index("shard")
        self.z, self.y = self.s // ys, lax.rem(self.s, ys)
        self.core = lax.rem(self.r, 2)
        self.xp = lax.rem(self.r // 2, 2)
        self.sib = (self.r + 1 - 2 * self.core, self.s)
        self.par = (self.r + 2 - 4 * self.xp, self.s)
        self.ypeers = [lax.rem(self.y + k, ys) for k in range(1, ys)]

    def at_z(self, off):
        return lax.rem(self.z + off, self.zs)

    def barrier(self):
        peers = [(self.r, self.at_z(k) * self.ys + self.y) for k in range(1, self.zs)]
        peers += [(self.r, self.z * self.ys + v) for v in self.ypeers] + [self.par, self.sib]
        bar = pltpu.get_barrier_semaphore()
        for p in peers:
            pl.semaphore_signal(bar, inc=1, device_id=p, device_id_type=MESH)
        pl.semaphore_wait(bar, len(peers))

    def geom(self, t, dest_z):
        w, offs, rows, c0, cols, turn = self.chunks[t]
        a = share_rows(rows)
        half = cols // 2
        mine = pl.ds(pl.multiple_of(self.xp * a, 16), rows - a)
        excl = pl.ds(pl.multiple_of(self.xp * (rows - a), 16), a)
        missing = pl.ds(pl.multiple_of((1 - self.xp) * (rows - a), 16), a)
        first = c0 + self.core * half
        if turn is not None:
            k, span = turn
            first = first + lax.rem(dest_z + k, self.zs) * span
        return w, offs, rows, a, half, mine, excl, missing, pl.ds(pl.multiple_of(first, 128), half)

    def send(self, src, w, zz, yy, rows, col, t, stage, device):
        pltpu.make_async_remote_copy(
            src_ref=src, dst_ref=self.lands[w].at[zz, yy, rows, col], send_sem=self.sems[2 * stage].at[t],
            recv_sem=self.sems[2 * stage + 1].at[t], device_id=device, device_id_type=MESH,
        ).start()

    def relay(self, w, zz, yy, rows, col, t, stage, device):
        self.send(self.lands[w].at[zz, yy, rows, col], w, zz, yy, rows, col, t, stage, device)

    def wait(self, t, stage, side):
        w, offs, rows, a, half, *_ = self.geom(t, self.z)
        far = len([o for o in offs if o])
        near = len(offs) * (self.ys - 1)
        count = ((far * (rows - a)), near * (rows - a), (far + near) * a, (far + near) * rows)[stage]
        if count == 0:
            return
        sem = self.sems[2 * stage + side].at[t]
        elems = count * half
        for out in self.lands:
            _, _, big_r, big_n = out.shape
            for lead in range(1, self.zs + 1):
                for take in range(big_r, 0, -16):
                    if elems % (lead * take * 128) == 0 and elems // (lead * take) <= big_n:
                        reg = out.at[pl.ds(0, lead), 0, pl.ds(0, take), pl.ds(0, elems // (lead * take))]
                        pltpu.make_async_copy(reg, reg, sem).wait()
                        return
        raise ValueError("no region")

    def start_z(self, t):
        offs = self.chunks[t][1]
        for k in range(1, self.zs):
            if (self.zs - k) % self.zs in offs:
                zz = self.at_z(k)
                w, _, _, _, _, mine, _, _, col = self.geom(t, zz)
                self.send(self.shards[w].at[mine, col], w, self.z, self.y, mine, col, t, 0, (self.r, zz * self.ys + self.y))

    def start_y(self, t):
        w, offs, _, _, _, mine, _, _, col = self.geom(t, self.z)
        if 0 in offs:
            for v in self.ypeers:
                self.send(self.shards[w].at[mine, col], w, self.z, self.y, mine, col, t, 1, (self.r, self.z * self.ys + v))

    def begin(self):
        for t in self.ahead[-1]:
            self.start_z(t)
            self.start_y(t)

    def relay_z(self, m):
        for t in self.ahead[m]:
            self.start_z(t)
            self.start_y(t)
        w, offs, rows, a, half, mine, excl, missing, col = self.geom(m, self.z)
        self.wait(m, 0, 1)
        for o in offs:
            if o:
                for v in self.ypeers:
                    self.relay(w, self.at_z(o), self.y, mine, col, m, 1, (self.r, self.z * self.ys + v))
        for o in offs:
            if o:
                self.relay(w, self.at_z(o), self.y, excl, col, m, 2, self.par)
                self.relay(w, self.at_z(o), self.y, mine, col, m, 3, self.sib)

    def relay_y(self, m):
        w, offs, rows, a, half, mine, excl, missing, col = self.geom(m, self.z)
        self.wait(m, 1, 1)
        for zz in [self.at_z(o) for o in offs]:
            for v in self.ypeers:
                self.relay(w, zz, v, excl, col, m, 2, self.par)
                self.relay(w, zz, v, mine, col, m, 3, self.sib)

    def relay_x(self, m):
        w, offs, rows, a, half, mine, excl, missing, col = self.geom(m, self.z)
        self.wait(m, 2, 1)
        for o in offs:
            if o:
                self.relay(w, self.at_z(o), self.y, missing, col, m, 3, self.sib)
        for zz in [self.at_z(o) for o in offs]:
            for v in self.ypeers:
                self.relay(w, zz, v, missing, col, m, 3, self.sib)

    def tick(self, todo):
        for stage, m in todo:
            (self.relay_z, self.relay_y, self.relay_x)[stage](m)

    def arrived(self, t):
        self.wait(t, 3, 1)

    def sent(self, t):
        for stage in range(4):
            self.wait(t, stage, 0)


QKV, ADN, AUP, OUT, UP, DOWN = range(6)
AHEAD = 6
WIDE = 1024
UNIT = (4.1, 3.9, 4.0)


def starts(sizes):
    out, nxt, open_now = {}, 0, 0
    for m in range(-1, len(sizes)):
        open_now -= sizes[m] if m >= 0 else 0
        out[m] = []
        while nxt < len(sizes) and open_now + sizes[nxt] <= AHEAD:
            open_now += sizes[nxt]
            out[m].append(nxt)
            nxt += 1
    return out


class Plan:
    def __init__(self, groups, pairs, zs, n_rb, sizes, outs):
        self.pairs = pairs
        n = len(sizes)
        self.ahead = starts(sizes)
        self.proj, self.att = [], []
        cost = [5.0, 3.0]
        need = {1: [0, 1]}
        for g in range(groups):
            for k in range(3):
                self.proj.append(len(cost))
                need[len(cost)] = [2 + 3 * g + k]
                cost.append(3.3)
            self.att.append(len(cost))
            cost += [3.45] * pairs
        done = 2 + 3 * groups
        self.out = len(cost)
        need[self.out] = list(range(done, done + outs))
        cost.append(6.0)
        done += outs
        self.ff = len(cost)
        per = (n - done) // zs
        for f in range(zs):
            need[len(cost)] = list(range(done + f * per, done + (f + 1) * per))
            cost += [3.6] * n_rb
        self.end = len(cost)
        cost += [3.6] * n_rb
        self.steps = len(cost)
        self.ticks = {}
        self.spread(cost, need, n, sizes)

    def spread(self, cost, need, n, sizes):
        hop, now = 1.5, 2.0
        free = [now, now, now]
        due = [{}, {}, {}]
        nxt = [0, 0, 0]
        ready = {}

        def begin(c, t):
            free[0] = max(free[0], t) + UNIT[0] * sizes[c]
            due[0][c] = free[0] + hop
            free[1] = max(free[1], t) + UNIT[1] * sizes[c] / 4

        def run(stage, t):
            c = nxt[stage]
            nxt[stage] += 1
            if stage == 0:
                for k in self.ahead[c]:
                    begin(k, t)
                free[1] = max(free[1], t) + UNIT[1] * 0.75 * sizes[c]
                due[1][c] = free[1] + hop
                free[2] = max(free[2], t) + UNIT[2] * 0.43 * sizes[c]
            elif stage == 1:
                free[2] = max(free[2], t) + UNIT[2] * 0.57 * sizes[c]
                due[2][c] = free[2] + hop
            else:
                ready[c] = t + 2.0
            return (stage, c)

        def open_ops():
            return [(due[k][nxt[k]], k) for k in range(3) if nxt[k] in due[k]]

        for c in self.ahead[-1]:
            begin(c, now)
        for step, spent in enumerate(cost):
            todo = []
            if step:
                wanted = need.get(step, [])
                if step == len(cost) - 1:
                    wanted = range(n)
                while True:
                    ops = [v for v in open_ops() if v[0] <= now]
                    if not ops:
                        if all(c in ready for c in wanted):
                            break
                        ops = open_ops()
                    at, stage = min(ops)
                    now = max(now, at)
                    todo.append(run(stage, now))
                for c in wanted:
                    now = max(now, ready[c])
            if todo:
                self.ticks[step] = todo
            now += spent
        self.estimate = now


def layer_body(
    zs, ys, tile, chunks, plan, n_rb, len_ref, id_ref, x_ref, cot_ref, g1_ref, g_ref, qkv_s, adn_s, aup_s, out_s, up_s, down_s,
    qkv_f, proj_ref, inner_ref, adn_ref, aup_ref, ctx_ref, p_ref, y_ref, gh_ref, gc_ref, dgrad_ref, ugrad_ref,
    qa, qb, out_v, up_v, down_v, hid, mlp_acc, gn_acc, nt, io, local, qsem, *sems,
):
    step = pl.program_id(0)
    seq, dim = x_ref.shape
    rows = seq // n_rb
    span = up_v.shape[3] // zs
    mover = Mover(zs, ys, (qkv_s, adn_s, aup_s, out_s, up_s, down_s), (qkv_f, qa, qb, out_v, up_v, down_v), sems, chunks, plan.ahead)
    own = [
        pltpu.make_async_copy(src, land.at[mover.z, mover.y], local.at[i])
        for i, (src, land) in enumerate(zip(mover.shards, mover.lands))
    ]

    @pl.when(step == 0)
    def _():
        for cp in own:
            cp.start()
        mover.barrier()
        mover.begin()

        def one(i, carry):
            sl = pl.ds(pl.multiple_of(i * rows, rows), rows)
            unit, _ = norm_stats(x_ref[sl, :].astype(F32))
            nt[sl, :] = (unit * g1_ref[...]).astype(BF)
            return carry

        lax.fori_loop(0, n_rb, one, 0)
        for cp in own:
            cp.wait()

    for at, todo in plan.ticks.items():

        @pl.when(step == at)
        def _():
            mover.tick(todo)

    @pl.when(step == 1)
    def _():
        for t in range(2):
            mover.arrived(t)
        wide = qa.shape[3]
        pick = lax.broadcasted_iota(jnp.int32, (wide, COLS), 0) == lax.broadcasted_iota(jnp.int32, (wide, COLS), 1) + id_ref[0] * COLS
        pick = jnp.where(pick, 1.0, 0.0).astype(BF)
        adn_ref[...] = dense(qa[...].reshape(dim, wide), pick).astype(BF)
        aup_ref[...] = dense(qb[...].reshape(dim, wide), pick).astype(BF)
        inner_ref[...] = dense(nt[...], adn_ref[...]).astype(BF)
        for t in range(2):
            mover.sent(t)

    part = qa.shape[3]
    for i, at in enumerate(plan.proj):
        c0 = (i % 3) * dim + (i // 3) * part
        buf = (qa, qb)[i % 2]

        @pl.when(step == at)
        def _():
            mover.arrived(2 + i)
            cp = pltpu.make_async_copy(qkv_f.at[:, :, :, pl.ds(c0, part)], buf, qsem)
            cp.start()
            cp.wait()

            def one(b, carry):
                sl = pl.ds(pl.multiple_of(b * rows, rows), rows)
                w = buf[...].reshape(dim, part)
                inner = lane_group(inner_ref[sl, :], RANK, i % 3)
                proj_ref[sl, pl.ds(c0, part)] = (
                    dense(nt[sl, :], w) + dense_trans(inner, aup_ref[pl.ds((i // 3) * part, part), :])
                ).astype(BF)
                return carry

            lax.fori_loop(0, n_rb, one, 0)

    lanes = dim // (plan.pairs * len(plan.att))
    for g, base in enumerate(plan.att):

        @pl.when((step >= base) & (step < base + plan.pairs))
        def _():
            first = (step - base + g * plan.pairs) * lanes

            def cut(ref, third):
                return ref.at[:, pl.ds(pl.multiple_of(third * dim + first, 128), lanes)]

            attn_fwd_body(tile, cut(proj_ref, 0), cut(proj_ref, 1), cut(proj_ref, 2), cut(ctx_ref, 0), p_ref)

    def valid_rows(first):
        return first + lax.broadcasted_iota(jnp.int32, (rows, 1), 0) < len_ref[0]

    @pl.when(step == plan.out)
    def _():
        for t in range(len(chunks)):
            if chunks[t][0] == OUT:
                mover.arrived(t)

        def one(i, carry):
            sl = pl.ds(pl.multiple_of(i * rows, rows), rows)
            ctx = ctx_ref[sl, :]
            inner_out = lane_group(dense(ctx, adn_ref[...]), RANK, 3).astype(BF)
            io[sl, :] = inner_out
            hidden = x_ref[sl, :].astype(F32) + (dense(ctx, out_v[...].reshape(dim, dim)) + dense_trans(inner_out, aup_ref[...]))
            hid[sl, :] = hidden
            unit, _ = norm_stats(hidden)
            nt[sl, :] = (unit * g_ref[...]).astype(BF)
            return carry

        lax.fori_loop(0, n_rb, one, 0)

    for k in range(zs):

        @pl.when(step == plan.ff + k * n_rb)
        def _():
            for t in range(len(chunks)):
                if chunks[t][0] == DOWN and chunks[t][1] == (k,) or chunks[t][0] == UP and chunks[t][5][0] == k:
                    mover.arrived(t)

    @pl.when((step >= plan.ff) & (step < plan.end))
    def _():
        at = step - plan.ff
        fz = lax.rem(mover.z + at // n_rb, zs)
        first = lax.rem(at, n_rb) * rows
        sl = pl.ds(pl.multiple_of(first, rows), rows)
        cot = cot_ref[...]
        grad_mlp = jnp.where(valid_rows(first), cot, jnp.zeros_like(cot))
        sub = min(512, span)
        shard_rows = down_v.shape[2]
        k0 = 0.7978845608028654
        for h in range(span // sub):
            up_w = up_v[:, :, :, pl.ds(pl.multiple_of(fz * span + h * sub, 128), sub)].reshape(dim, sub)
            per = sub // shard_rows
            if per:
                down_w = down_v[fz, pl.ds(h * per, per)].reshape(sub, dim)
            else:
                down_w = down_v[fz, h * sub // shard_rows, pl.ds(h * sub % shard_rows, sub)]
            u = dense(nt[sl, :], up_w)
            ga = dense_trans(grad_mlp, down_w)
            sq = u * u
            t = jnp.tanh(k0 * (u + 0.044715 * u * sq))
            half = 0.5 * (1.0 + t)
            act = (u * half).astype(BF)
            d = half + 0.5 * u * (1.0 - t * t) * (k0 * (1.0 + (3.0 * 0.044715) * sq))
            gp = (ga * d).astype(BF)
            m_new = dense(act, down_w)
            g_new = dense_trans(gp, up_w)
            if h == 0:

                @pl.when(at < n_rb)
                def _():
                    mlp_acc[sl, :] = m_new
                    gn_acc[sl, :] = g_new

                @pl.when(at >= n_rb)
                def _():
                    mlp_acc[sl, :] += m_new
                    gn_acc[sl, :] += g_new
            else:
                mlp_acc[sl, :] += m_new
                gn_acc[sl, :] += g_new

    @pl.when(step >= plan.end)
    def _():
        first = (step - plan.end) * rows
        sl = pl.ds(pl.multiple_of(first, rows), rows)
        valid = valid_rows(first)
        hidden = hid[sl, :]
        cot = cot_ref[...]
        y_ref[...] = jnp.where(valid, hidden + mlp_acc[sl, :], 0.0).astype(BF)
        unit, rs = norm_stats(hidden)
        gh = jnp.where(valid, cot, jnp.zeros_like(cot)).astype(F32) + norm_back(unit, rs, g_ref[...], gn_acc[sl, :])
        gh_ref[...] = gh
        ga = gh.astype(BF)
        gio = lane_group(dense(ga, aup_ref[...]), RANK, 3).astype(BF)
        gc_ref[...] = (dense_trans(ga, out_v[...].reshape(dim, dim)) + dense_trans(gio, adn_ref[...])).astype(BF)

        @pl.when(step == plan.end)
        def _():
            dgrad_ref[...] = jnp.zeros_like(dgrad_ref)
            ugrad_ref[...] = jnp.zeros_like(ugrad_ref)

        dgrad_ref[...] += dense_left(gio, ctx_ref[sl, :])
        ugrad_ref[...] += dense_left(io[sl, :], ga)

    @pl.when(step == pl.num_programs(0) - 1)
    def _():
        for t in range(2, len(chunks)):
            mover.sent(t)


def layer(length, adapter, x, cot, gain_one, gain_two, shard_set, n_rep, n_shard, tile, lanes=128, n_rb=4):
    zs, ys = mesh_split(n_rep, n_shard)
    qkv_s, adn_s, aup_s, out_s, up_s, down_s = shard_set
    seq, dim = x.shape
    ff = up_s.shape[1]
    heads = lanes // HEAD
    packed = tile * (seq // tile) * (seq // tile + 1) // 2
    rows = seq // n_rb
    span = ff // zs
    every = tuple(range(zs))
    part = adn_s.shape[1]
    chunks = [(w, every, adn_s.shape[0], 0, part, None) for w in (ADN, AUP)]
    for c in range(0, dim, part):
        chunks += [(QKV, every, qkv_s.shape[0], k * dim + c, part, None) for k in range(3)]
    wide = min(WIDE, dim, span)
    chunks += [(OUT, every, out_s.shape[0], c, wide, None) for c in range(0, dim, wide)]
    for k in range(zs):
        chunks += [(DOWN, (k,), down_s.shape[0], c, wide, None) for c in range(0, dim, wide)]
        chunks += [(UP, every, up_s.shape[0], c, wide, (k, span)) for c in range(0, span, wide)]
    n = len(chunks)
    sizes = [c[4] // part for c in chunks]
    plan = Plan(dim // part, part // lanes, zs, n_rb, sizes, dim // wide)

    def whole(shape):
        return pl.BlockSpec(shape, lambda j: (0, 0), pipeline_mode=pl.Buffered(1))

    def late(j):
        return (jnp.maximum(j - plan.end, 0), 0)

    def pair(j):
        at = jnp.minimum(jnp.maximum(j - plan.att[0], 0), plan.pairs - 1)
        for base in plan.att[1:]:
            at = at + jnp.minimum(jnp.maximum(j - base + 1, 0), plan.pairs)
        return (at, 0, 0)

    row = pl.BlockSpec((rows, dim), late)
    hbm = pl.BlockSpec(memory_space=pl.ANY)
    smem = pl.BlockSpec(memory_space=pltpu.SMEM)
    return pl.pallas_call(
        functools.partial(layer_body, zs, ys, tile, chunks, plan, n_rb),
        grid=(plan.steps,),
        out_shape=[
            jax.ShapeDtypeStruct((zs, ys) + qkv_s.shape, BF),
            jax.ShapeDtypeStruct((seq, 3 * dim), BF),
            jax.ShapeDtypeStruct((seq, COLS), BF),
            jax.ShapeDtypeStruct((dim, COLS), BF),
            jax.ShapeDtypeStruct((dim, COLS), BF),
            jax.ShapeDtypeStruct((seq, dim), BF),
            jax.ShapeDtypeStruct((dim // HEAD, tile, packed), BF),
            jax.ShapeDtypeStruct((seq, dim), BF),
            jax.ShapeDtypeStruct((seq, dim), F32),
            jax.ShapeDtypeStruct((seq, dim), BF),
            jax.ShapeDtypeStruct((COLS, dim), F32),
            jax.ShapeDtypeStruct((COLS, dim), F32),
        ],
        in_specs=[
            smem, smem, whole((seq, dim)),
            pl.BlockSpec((rows, dim), lambda j: (lax.rem(jnp.maximum(j - plan.ff, 0), n_rb), 0)),
            whole((1, dim)), whole((1, dim)), pl.BlockSpec(memory_space=pltpu.VMEM),
            hbm, hbm, hbm, hbm, hbm,
        ],
        out_specs=[
            hbm, whole((seq, 3 * dim)), whole((seq, COLS)), whole((dim, COLS)), whole((dim, COLS)), whole((seq, dim)),
            pl.BlockSpec((heads, tile, packed), pair),
            row, row, row, whole((COLS, dim)), whole((COLS, dim)),
        ],
        scratch_shapes=[
            pltpu.VMEM((zs, ys) + adn_s.shape, BF),
            pltpu.VMEM((zs, ys) + aup_s.shape, BF),
            pltpu.VMEM((zs, ys) + out_s.shape, BF),
            pltpu.VMEM((zs, ys) + up_s.shape, BF),
            pltpu.VMEM((zs, ys) + down_s.shape, BF),
            pltpu.VMEM((seq, dim), F32),
            pltpu.VMEM((seq, dim), F32),
            pltpu.VMEM((seq, dim), F32),
            pltpu.VMEM((seq, dim), BF),
            pltpu.VMEM((seq, COLS), BF),
            pltpu.SemaphoreType.DMA((6,)),
            pltpu.SemaphoreType.DMA,
        ]
        + [pltpu.SemaphoreType.DMA((n,))] * 8,
        compiler_params=pltpu.CompilerParams(collective_id=0, has_side_effects=True, vmem_limit_bytes=66_500_000),
        name="layer_with_gather",
    )(length, adapter, x, cot, gain_one, gain_two, qkv_s, adn_s, aup_s, out_s, up_s, down_s)


def one_slot(tokens, slot_cot, length, adapter, shard_set, gain_one, gain_two, n_rep, n_shard):
    tile = 256 if tokens.shape[0] % 256 == 0 else tokens.shape[0]
    g_one, g_two = gain_one[None], gain_two[None]
    qkv, proj, inner, adn, aup, ctx, probs, y, gh, gc, dg, ug = layer(
        length, adapter, tokens, slot_cot, g_one, g_two, shard_set, n_rep, n_shard, tile
    )
    dq, dk, dv, y = attention_backward(proj, gc, ctx, probs, y, tile)
    qkv = qkv.reshape(-1, qkv.shape[-1])
    return y, *tail_backward(tokens, gh, inner, dq, dk, dv, g_one, qkv, adn, aup, dg, ug, adapter, n_rep, n_shard)


PAY = 2 * COLS + 16


def flip(value, bit):
    return value + bit - 2 * bit * lax.rem(value // bit, 2)


def tail_body(
    n_rep, n_shard, bits, nb, x_ref, gh_ref, inner_ref, dq_ref, dk_ref, dv_ref, g_ref, w_ref, adn_ref, aup_ref,
    din_ref, uin_ref, id_ref, gx_ref, down_ref, up_ref, gi_s, dgrad, ugrad, pay, buf, send, recv, xsend, xrecv, lsem,
):
    step = pl.program_id(0)
    rows, dim = x_ref.shape
    r = lax.axis_index("rep")
    s = lax.axis_index("shard")
    others = [lax.rem(s + k, n_shard) for k in range(1, n_shard)]
    peers = [(r, o) for o in others] + [(flip(r, b), s) for b in bits]
    own = pltpu.make_async_copy(pay.at[s], buf.at[r, s], lsem)
    first = [
        pltpu.make_async_remote_copy(
            src_ref=pay.at[o], dst_ref=buf.at[r, s], send_sem=send.at[k], recv_sem=recv.at[k],
            device_id=(r, o), device_id_type=MESH,
        )
        for k, o in enumerate(others)
    ]
    rounds = []
    held, at = [0], 0
    for b in bits:
        copies = []
        for m in held:
            q = r
            for c in bits:
                if m & c:
                    q = flip(q, c)
            copies.append(
                pltpu.make_async_remote_copy(
                    src_ref=buf.at[q], dst_ref=buf.at[q], send_sem=xsend.at[at], recv_sem=xrecv.at[at],
                    device_id=(flip(r, b), s), device_id_type=MESH,
                )
            )
            at += 1
        rounds.append(copies)
        held = held + [m | b for m in held]

    def block_sl():
        return pl.ds(pl.multiple_of(lax.rem(step, nb) * rows, rows), rows)

    @pl.when(step == 0)
    def _():
        dgrad[...] = din_ref[...]
        ugrad[...] = uin_ref[...]

    @pl.when(step < nb)
    def _():
        thirds = [dq_ref[...], dk_ref[...], dv_ref[...]]
        gi, up = None, None
        for p in range(3):
            one = lane_group(dense(thirds[p], aup_ref[...]), RANK, p)
            gi = one if gi is None else gi + one
            two = dense_left(lane_group(inner_ref[...], RANK, p), thirds[p])
            up = two if up is None else up + two
        gi = gi.astype(BF)
        gi_s[block_sl(), :] = gi
        unit, _ = norm_stats(x_ref[...].astype(F32))
        dgrad[...] += dense_left(gi, (unit * g_ref[...]).astype(BF))
        ugrad[...] += up

    @pl.when(step == nb - 1)
    def _():
        width = pay.shape[2]
        mark = jnp.full((PAY - 2 * COLS, width), id_ref[0], jnp.int32).astype(F32)
        for i in range(n_shard):
            sl = pl.ds(i * width, width)
            pay[i] = jnp.concatenate([dgrad[:, sl], ugrad[:, sl], mark], axis=0).astype(BF)
        bar = pltpu.get_barrier_semaphore()
        for p in peers:
            pl.semaphore_signal(bar, inc=1, device_id=p, device_id_type=MESH)
        pl.semaphore_wait(bar, len(peers))

    @pl.when(step == nb)
    def _():
        own.start()
        for cp in first:
            cp.start()

    @pl.when(step == nb + nb // 2)
    def _():
        own.wait()
        for cp in first:
            cp.wait()
        for cp in rounds[0]:
            cp.start()

    @pl.when((step >= nb) & (step < 2 * nb))
    def _():
        thirds = [dq_ref[...], dk_ref[...], dv_ref[...]]
        gn = dense_trans(gi_s[block_sl(), :], adn_ref[...])
        for p in range(3):
            gn = gn + dense_trans(thirds[p], w_ref[:, pl.ds(p * dim, dim)])
        unit, rs = norm_stats(x_ref[...].astype(F32))
        gx_ref[...] = (gh_ref[...] + norm_back(unit, rs, g_ref[...], gn)).astype(BF)

    @pl.when(step == 2 * nb)
    def _():
        for cp in rounds[0]:
            cp.wait()
        for copies in rounds[1:]:
            for cp in copies:
                cp.start()
            for cp in copies:
                cp.wait()
        width = buf.shape[3]
        for a in range(ADAPTERS):

            def add(i, acc):
                low = buf[i // n_shard, lax.rem(i, n_shard)]
                block = low[: 2 * COLS, :].astype(F32)
                mark = low[2 * COLS : 2 * COLS + 8, :].astype(F32)[0:1, :]
                return acc + jnp.where(mark == float(a), block, 0.0)

            total = lax.fori_loop(0, n_rep * n_shard, add, jnp.zeros((2 * COLS, width), F32), unroll=4)
            flat = jnp.transpose(total)
            down_ref[:, pl.ds(a * COLS, COLS)] = flat[:, :COLS]
            up_ref[:, pl.ds(a * COLS, COLS)] = flat[:, COLS:]


def tail_backward(x, gh, inner, dq, dk, dv, gain, qkv, adn, aup, din, uin, adapter, n_rep, n_shard, rows=256):
    seq, dim = x.shape
    nb = seq // rows
    bits = [1 << k for k in range(1, n_rep.bit_length() - 1)] + [1]
    width = dim // n_shard

    def both(j):
        return (lax.rem(jnp.minimum(j, 2 * nb - 1), nb), 0)

    def second(j):
        return (jnp.minimum(jnp.maximum(j - nb, 0), nb - 1), 0)

    def whole(shape):
        return pl.BlockSpec(shape, lambda j: (0, 0), pipeline_mode=pl.Buffered(1))

    row = pl.BlockSpec((rows, dim), both)
    late = pl.BlockSpec((rows, dim), second)
    return pl.pallas_call(
        functools.partial(tail_body, n_rep, n_shard, bits, nb),
        grid=(2 * nb + 1,),
        out_shape=[jax.ShapeDtypeStruct((seq, dim), BF)]
        + [jax.ShapeDtypeStruct((width, ADAPTERS * COLS), F32)] * 2,
        in_specs=[
            row, late, pl.BlockSpec((rows, COLS), both), row, row, row,
            whole((1, dim)), whole(qkv.shape), whole((dim, COLS)), whole((dim, COLS)), whole((COLS, dim)), whole((COLS, dim)),
            pl.BlockSpec(memory_space=pltpu.SMEM),
        ],
        out_specs=[late, whole((width, ADAPTERS * COLS)), whole((width, ADAPTERS * COLS))],
        scratch_shapes=[
            pltpu.VMEM((seq, COLS), BF),
            pltpu.VMEM((COLS, dim), F32),
            pltpu.VMEM((COLS, dim), F32),
            pltpu.VMEM((n_shard, PAY, width), BF),
            pltpu.VMEM((n_rep, n_shard, PAY, width), BF),
        ]
        + [pltpu.SemaphoreType.DMA((n_shard - 1,))] * 2
        + [pltpu.SemaphoreType.DMA((n_rep - 1,))] * 2
        + [pltpu.SemaphoreType.DMA],
        compiler_params=pltpu.CompilerParams(collective_id=1, has_side_effects=True, vmem_limit_bytes=VMEM_CAP),
        name="tail_and_reduce",
    )(x, gh, inner, dq, dk, dv, gain, qkv, adn, aup, din, uin, adapter)


def shards(
    inputs,
    cotangent,
    lengths,
    adapter_ids,
    gain_one,
    gain_two,
    qkv_weight,
    out_weight,
    up_weight,
    down_weight,
    adapter_down,
    adapter_up,
):
    n_rep, n_shard = lax.axis_size("rep"), lax.axis_size("shard")
    shard_set = (qkv_weight, adapter_down, adapter_up, out_weight, up_weight, down_weight)
    output, grad, down_grad, up_grad = one_slot(
        inputs[0], cotangent[0], lengths, adapter_ids, shard_set, gain_one, gain_two, n_rep, n_shard
    )
    return (output[None], grad[None], down_grad, up_grad)


def solution(mesh):
    return jax.shard_map(
        shards,
        mesh=mesh,
        in_specs=(
            P(("rep", "shard"), None, None),
            P(("rep", "shard"), None, None),
            P(("rep", "shard")),
            P(("rep", "shard")),
            P(),
            P(),
            P("shard", None),
            P("shard", None),
            P("shard", None),
            P("shard", None),
            P("shard", None),
            P("shard", None),
        ),
        out_specs=(
            P(("rep", "shard"), None, None),
            P(("rep", "shard"), None, None),
            P("shard", None),
            P("shard", None),
        ),
        check_vma=False,
    )
```
